32 devices in a mesh: node: 16 (over z, x, core), local: 2 (over y).
Axes of the slice: x: 2, y: 2, z: 4, core: 2. Of those that a mesh axis runs over, the one named last changes fastest.
Arguments:
- hidden: bfloat16 [2, 4096, 4096], P('local', 'node'), may hold values from -6 to 6
- queries: bfloat16 [2, 4096, 2048], P('local', 'node'), may hold values from -30 to 30
- saved_keys: bfloat16 [2, 4096, 512], P('local', 'node'), may hold values from -30 to 30
- grad_out: bfloat16 [2, 4096, 2048], P('local', 'node'), may hold values from -6 to 6
- value_weight: bfloat16 [4096, 512], P('local'), may hold values from -0.09375 to 0.09375
- doc_lengths: int32 [2, 16], P('local'), may hold values from 0 to 1024, as said below
- doc_order: int32 [2, 16], P('local'), may hold values from 0 to 15, each once within a row
Outputs:
- query_grad: bfloat16 [2, 4096, 2048], P('local', 'node')
- key_grad: bfloat16 [2, 4096, 512], P('local', 'node')
- input_grad: bfloat16 [2, 4096, 4096], P('local', 'node')
- weight_grad: float32 [4096, 512], P(('node', 'local'))
The draws below stay inside these ranges and needn't reach their ends.
Inputs may be any that keep to these rules, and one draw needn't show every extreme that they name: `doc_lengths`: a document occupies ceil(length / 256) whole blocks, at most 4; the documents of a sequence fill its 16 blocks exactly; in every sequence some document takes 4 blocks.
All inputs are finite; a program needn't handle non-finite values.
Results may differ from the reference program's by a relative error of at most 0.0085.
Values may be sent and summed in bfloat16 or wider, within the bound.
A program may use at most 128 MiB of HBM per device.

```python
import jax
import jax.numpy as jnp
from jax import lax

D = 4096
HD = 128
KVH = 4
GROUP = 4
BLOCK = 256
DOCB = 4
QW = 2048
KVW = 512
NBLK = 16
SEQLEN = 4096
SEQS = 2


def paired_rows(key):
    base = jax.random.fold_in(key, 17)
    key_query, key_keys = jax.random.split(base)
    query_draw = jnp.clip(jax.random.normal(key_query, (SEQS, SEQLEN, QW), jnp.float32), -6.0, 6.0)
    key_draw = jnp.clip(jax.random.normal(key_keys, (SEQS, SEQLEN, KVW), jnp.float32), -6.0, 6.0)
    return (query_draw, key_draw)


def draw_queries(key, part):
    return paired_rows(key)[0].astype(jnp.bfloat16)


def draw_saved_keys(key, part):
    return paired_rows(key)[1].astype(jnp.bfloat16)


def draw_doc_lengths(key, part):
    key_count, key_len = jax.random.split(jax.random.fold_in(key, 3))
    counts = jax.random.randint(key_count, (SEQS, NBLK), 1, DOCB + 1)
    counts = counts.at[:, 1].set(DOCB)
    ends = jnp.cumsum(counts, axis=1)
    starts = ends - counts
    living = starts < NBLK
    counts = jnp.where(living, jnp.minimum(counts, NBLK - starts), 0)
    extra = jax.random.randint(key_len, (SEQS, NBLK), 1, BLOCK + 1)
    return jnp.where(living, (counts - 1) * BLOCK + extra, 0).astype(jnp.int32)


def strengthened(values, key, source, target, parts, factor):
    def block_of(position):
        return (jnp.arange(values.shape[position]) // (values.shape[position] // parts)).reshape((-1,) + (1,) * (values.ndim - 1 - position))

    near = jax.random.permutation(key, parts)[block_of(target)]
    second = (block_of(target) + parts // 2) % parts
    return jnp.where((block_of(source) == near) | (block_of(source) == second), factor * values, values)


def block_scale(rng, dims, cuts, smallest, largest):
    loudness, own = 1.0, jax.random.fold_in(rng, 6)
    for dim, parts in cuts:
        draws = jnp.exp(jax.random.uniform(jax.random.fold_in(own, dim), (parts,), jnp.float32, smallest / len(cuts), largest / len(cuts)))
        loudness = loudness * jnp.repeat(draws, dims[dim] // parts).reshape([-1 if axis == dim else 1 for axis in range(len(dims))])
    return loudness


def normal_values(stream_key, extent, spread, limit, shards=(), held_as=jnp.bfloat16):
    gain = block_scale(stream_key, extent, shards, -0.22, 0.18) if shards else 1.0
    entries = jax.random.normal(stream_key, extent, jnp.float32) * spread * gain
    return jnp.minimum(jnp.maximum(entries, -limit), limit).astype(held_as)


def gaussian_with(key, shape, deviation, most, cuts, heavy, kind=jnp.bfloat16):
    result = deviation * jax.random.normal(key, shape, jnp.float32)
    if cuts:
        result = result * block_scale(key, shape, cuts, -0.22, 0.18)
    return jnp.clip(strengthened(result, jax.random.fold_in(key, 3), *heavy), -most, most).astype(kind)


def setup_inputs(seed: int = 0) -> dict:
    arg_keys = jax.random.split(jax.random.key(seed), 8)
    hidden = gaussian_with(arg_keys[0], (SEQS, SEQLEN, D), 1.0, 6.0, ((0, 2), (1, 16)), (1, 2, 16, 2.0))
    queries = draw_queries(jax.random.fold_in(arg_keys[7], 71), 0)
    saved_keys = draw_saved_keys(jax.random.fold_in(arg_keys[7], 71), 0)
    grad_out = normal_values(arg_keys[3], (SEQS, SEQLEN, QW), 1.0, 6.0, ((0, 2), (1, 16)))
    value_weight = normal_values(arg_keys[4], (D, KVW), D ** -0.5, 0.09375, ((0, 2),))
    doc_lengths = draw_doc_lengths(jax.random.fold_in(arg_keys[7], 71), 0)
    doc_order = jax.vmap(lambda own: jax.random.permutation(own, NBLK))(jax.random.split(arg_keys[6], SEQS)).reshape((SEQS, NBLK)).astype(jnp.int32)
    return {"hidden": hidden, "queries": queries, "saved_keys": saved_keys, "grad_out": grad_out, "value_weight": value_weight, "doc_lengths": doc_lengths, "doc_order": doc_order}


masked_score = -1e30


def doc_layout(lengths_row, order_row):
    slot_ids = jnp.arange(NBLK, dtype=jnp.int32)
    picked = order_row[:, None] == slot_ids[None, :]
    lens_ord = jnp.sum(jnp.where(picked, lengths_row[None, :], 0), axis=1).astype(jnp.int32)
    block_count = ((lens_ord + BLOCK - 1) // BLOCK).astype(jnp.int32)
    first_block = (jnp.cumsum(block_count) - block_count).astype(jnp.int32)
    return lens_ord, block_count, first_block


def block_info(block_index, lens_ord, block_count, first_block):
    member = (first_block <= block_index) & (block_index < first_block + block_count)
    has_doc = jnp.any(member)
    doc_start = jnp.sum(jnp.where(member, first_block, 0)).astype(jnp.int32)
    length = jnp.sum(jnp.where(member, lens_ord, 0)).astype(jnp.int32)
    return jnp.where(has_doc, doc_start, -1).astype(jnp.int32), length


def window_mask(block_index, layout):
    doc_start, length = block_info(block_index, *layout)
    inside = jnp.arange(BLOCK, dtype=jnp.int32)
    query_ok = (block_index - doc_start) * BLOCK + inside < length
    mask_parts = []
    for offset in range(DOCB - 1, -1, -1):
        other_block = block_index - offset
        other_start, other_len = block_info(other_block, *layout)
        key_ok = (other_start == doc_start) & ((other_block - doc_start) * BLOCK + inside < length)
        allowed = jnp.broadcast_to(key_ok[None, :], (BLOCK, BLOCK))
        if offset == 0:
            allowed = allowed & (inside[None, :] <= inside[:, None])
        mask_parts.append(allowed)
    return query_ok, jnp.concatenate(mask_parts, axis=1)


def tile_grads(query_rows, grad_rows, key_window, value_window, allowed):
    width = key_window.shape[0]
    score_scale = HD ** -0.5
    q_heads = query_rows.reshape(BLOCK, KVH, GROUP, HD).astype(jnp.float32)
    g_heads = grad_rows.reshape(BLOCK, KVH, GROUP, HD).astype(jnp.float32)
    k_heads = key_window.reshape(width, KVH, HD).astype(jnp.float32)
    v_heads = value_window.reshape(width, KVH, HD).astype(jnp.float32)
    scores = jnp.einsum("tgjd,wgd->gjtw", q_heads, k_heads) * score_scale
    scores = jnp.where(allowed[None, None], scores, masked_score)
    peak = jnp.max(scores, axis=3, keepdims=True)
    expd = jnp.exp(scores - peak)
    attn_probs = expd / jnp.sum(expd, axis=3, keepdims=True)
    attn_low = attn_probs.astype(jnp.bfloat16).astype(jnp.float32)
    attn_out = jnp.einsum("gjtw,wgd->tgjd", attn_low, v_heads)
    prob_grad = jnp.einsum("tgjd,wgd->gjtw", g_heads, v_heads)
    row_delta = jnp.einsum("tgjd,tgjd->gjt", g_heads, attn_out)
    score_grad = (attn_probs * (prob_grad - row_delta[..., None]) * score_scale).astype(jnp.bfloat16).astype(jnp.float32)
    query_grad = jnp.einsum("gjtw,wgd->tgjd", score_grad, k_heads).reshape(BLOCK, QW).astype(jnp.bfloat16)
    key_grad = jnp.einsum("gjtw,tgjd->wgd", score_grad, q_heads).reshape(width, KVW)
    value_grad = jnp.einsum("gjtw,tgjd->wgd", attn_low, g_heads).reshape(width, KVW)
    return query_grad, key_grad, value_grad


def gather_window(windows):
    pieces = windows.reshape(NBLK, DOCB, BLOCK, KVW)
    summed = jnp.zeros((NBLK + DOCB - 1, BLOCK, KVW), jnp.float32)
    for offset in range(DOCB):
        summed = summed.at[offset:offset + NBLK].add(pieces[:, offset])
    return summed[DOCB - 1:].reshape(SEQLEN, KVW)


def reference(hidden, queries, saved_keys, grad_out, value_weight, doc_lengths, doc_order):
    flat_hidden = hidden.reshape(SEQS * SEQLEN, D)
    values = jnp.dot(flat_hidden, value_weight, preferred_element_type=jnp.float32).astype(jnp.bfloat16)
    values = values.reshape(SEQS, SEQLEN, KVW)
    query_list, key_list, value_list = [], [], []
    for sequence in range(SEQS):
        layout = doc_layout(doc_lengths[sequence], doc_order[sequence])
        padding = jnp.zeros(((DOCB - 1) * BLOCK, KVW), jnp.bfloat16)
        key_padded = jnp.concatenate([padding, saved_keys[sequence]], axis=0)
        value_padded = jnp.concatenate([padding, values[sequence]], axis=0)
        seq_queries = queries[sequence]
        seq_grads = grad_out[sequence]

        def one_block(block_index):
            query_ok, allowed = window_mask(block_index, layout)
            first_row = (block_index * BLOCK).astype(jnp.int32)
            query_rows = lax.dynamic_slice_in_dim(seq_queries, first_row, BLOCK, 0)
            grad_rows = lax.dynamic_slice_in_dim(seq_grads, first_row, BLOCK, 0)
            grad_rows = grad_rows * query_ok[:, None].astype(grad_rows.dtype)
            key_window = lax.dynamic_slice_in_dim(key_padded, first_row, DOCB * BLOCK, 0)
            value_window = lax.dynamic_slice_in_dim(value_padded, first_row, DOCB * BLOCK, 0)
            return tile_grads(query_rows, grad_rows, key_window, value_window, allowed)

        block_query, block_key, block_value = lax.map(one_block, jnp.arange(NBLK, dtype=jnp.int32))
        query_list.append(block_query.reshape(SEQLEN, QW))
        key_list.append(gather_window(block_key))
        value_list.append(gather_window(block_value))
    query_grad = jnp.stack(query_list)
    key_grad = jnp.stack(key_list).astype(jnp.bfloat16)
    value_low = jnp.stack(value_list).astype(jnp.bfloat16).reshape(SEQS * SEQLEN, KVW)
    input_grad = jnp.dot(value_low, value_weight.T, preferred_element_type=jnp.float32).astype(jnp.bfloat16)
    weight_grad = jnp.dot(flat_hidden.T, value_low, preferred_element_type=jnp.float32)
    return query_grad, key_grad, input_grad.reshape(SEQS, SEQLEN, D), weight_grad
```

```python
import functools

import jax
import jax.numpy as jnp
from jax import lax
from jax.experimental import pallas as pl
from jax.experimental.pallas import tpu as pltpu
from jax.sharding import PartitionSpec as P

HD = 128
DOCB = 4
BF16 = jnp.bfloat16
F32 = jnp.float32
LOG2E = 1.4426950408889634
MESH = pl.DeviceIdType.MESH

masked_score = -1e30

ROWS_BY_ROWS = (((1,), (1,)), ((), ()))


def dot(a, b):
    return jnp.dot(a, b, preferred_element_type=F32)


def dot_rows(a, b):
    return lax.dot_general(a, b, ROWS_BY_ROWS, preferred_element_type=F32)


def remote(src, dst, send_sem, recv_sem, **where):
    return pltpu.make_async_remote_copy(
        src_ref=src,
        dst_ref=dst,
        send_sem=send_sem,
        recv_sem=recv_sem,
        device_id=where,
        device_id_type=MESH,
    )


def when(condition):
    if condition is True:
        return lambda body: body()
    return pl.when(condition)


def kernel(sizes, *refs):
    N, L, T, D, KVH, G = (sizes[k] for k in ("N", "L", "T", "D", "KVH", "G"))
    names = sizes["names"]
    r = dict(zip(names, refs))
    C = HD
    NZ = N // 4
    RO = D // (N * L)
    GW = D // N
    R = D // L
    QUARTER, SUB = R // 4, R // 16
    GC = G * C
    scale = HD ** (-0.5)

    n = lax.axis_index("node")
    l = lax.axis_index("local")
    core = lax.rem(n, 2)
    even, odd = core == 0, core == 1
    partner = n + 1 - 2 * core
    xbit = lax.rem(lax.div(n, 2), 2)
    xpeer = n + 2 - 4 * xbit
    z = lax.div(n, 4)
    zbit = lax.rem(z, 2)
    zpeer = n + 4 - 8 * zbit
    has_next, has_prev = n + 2 < N, n >= 2
    has_far_next, has_far_prev = n + 3 < N, n >= 3

    kwin, vwin = r["kwin"], r["vwin"]
    hid, hidp, hid_t, wfull = r["hid"], r["hidp"], r["hid_t"], r["wfull"]

    def rows(offset):
        return pl.ds((DOCB - 1 - offset) * T, T)

    for offset in range(1, DOCB):

        @pl.when(n < offset)
        def _():
            for win in (kwin, vwin):
                for kv in range(KVH):
                    win[kv, rows(offset)] = jnp.zeros((T, C), BF16)

    for name in ("v", "k"):

        @pl.when(n + 2 >= N)
        def _():
            r[name + "_near"][...] = jnp.zeros((KVH, T, C), BF16)

        @pl.when(jnp.logical_and(odd, n + 3 >= N))
        def _():
            r[name + "_third"][...] = jnp.zeros((KVH, T, C), BF16)

    def local_copy(src, dst, sem):
        return pltpu.make_async_copy(src, dst, sem)

    def key_in(kv):
        return local_copy(
            r["keys"].at[:, pl.ds(kv * C, C)], kwin.at[kv, rows(0)], r["key_in_sem"].at[kv]
        )

    def query_in(kv):
        cols = pl.ds(kv * GC, GC)
        return local_copy(r["queries"].at[:, cols], r["q"].at[kv], r["query_in_sem"].at[kv])

    def grad_in(kv):
        cols = pl.ds(kv * GC, GC)
        return local_copy(r["grads"].at[:, cols], r["g"].at[kv], r["grad_in_sem"].at[kv])

    hidden_in = local_copy(r["hidden"], hid, r["in_sem"].at[0])
    weight_in = local_copy(r["weight"], wfull.at[pl.ds(l * R, R)], r["in_sem"].at[1])
    for kv in range(KVH):
        key_in(kv).start()
    hidden_in.start()
    weight_in.start()
    for kv in range(KVH):
        query_in(kv).start()
        grad_in(kv).start()

    barrier = pltpu.get_barrier_semaphore()

    def greet(**where):
        pl.semaphore_signal(barrier, inc=1, device_id=where, device_id_type=MESH)

    greet(node=partner)
    for there, who in (
        (has_next, n + 2),
        (has_prev, n - 2),
        (jnp.logical_and(odd, has_far_next), n + 3),
        (jnp.logical_and(even, has_far_prev), n - 3),
    ):

        @pl.when(there)
        def _():
            greet(node=who)

    for s in range(1, L):
        greet(local=lax.rem(l + s, L))
    for s in range(1, NZ):
        greet(node=lax.rem(n + 4 * s, N))
    as_int = lambda b: jnp.where(b, 1, 0)
    expected = (
        1
        + as_int(has_next)
        + as_int(has_prev)
        + core * as_int(has_far_next)
        + (1 - core) * as_int(has_far_prev)
        + (L - 1)
        + (NZ - 1)
    )
    pl.semaphore_wait(barrier, expected)

    def window(win, name):
        send, recv = r[name + "_send"], r[name + "_recv"]

        def ahead(kv):
            return remote(
                win.at[kv, rows(0)], win.at[kv, rows(2)], send.at[0, kv], recv.at[1, kv], node=n + 2
            )

        def beside(kv):
            return remote(
                win.at[kv, rows(0)], win.at[kv, rows(1)], send.at[1, kv], recv.at[0, kv], node=n + 1
            )

        def far(kv):
            return remote(
                win.at[kv, rows(0)], win.at[kv, rows(3)], send.at[1, kv], recv.at[2, kv], node=n + 3
            )

        def relay_even(kv):
            return remote(
                win.at[kv, rows(2)], win.at[kv, rows(3)], send.at[2, kv], recv.at[2, kv], node=n + 1
            )

        def relay_odd(kv):
            return remote(
                win.at[kv, rows(2)], win.at[kv, rows(1)], send.at[2, kv], recv.at[0, kv], node=n - 1
            )

        far_there = jnp.logical_and(odd, has_far_next)
        relay_e = jnp.logical_and(even, has_prev)
        relay_o = jnp.logical_and(odd, has_prev)

        def start(kv):
            pl.when(has_next)(lambda: ahead(kv).start())
            pl.when(far_there)(lambda: far(kv).start())
            pl.when(even)(lambda: beside(kv).start())

        def relay(kv):
            @pl.when(has_prev)
            def _():
                ahead(kv).wait_recv()

            pl.when(relay_e)(lambda: relay_even(kv).start())
            pl.when(relay_o)(lambda: relay_odd(kv).start())

        def wait(kv):
            pl.when(jnp.logical_or(odd, has_prev))(lambda: beside(kv).wait_recv())
            pl.when(has_far_prev)(lambda: far(kv).wait_recv())

        def drain(kv):
            pl.when(has_next)(lambda: ahead(kv).wait_send())
            pl.when(jnp.logical_or(even, has_far_next))(lambda: far(kv).wait_send())
            pl.when(has_prev)(lambda: relay_even(kv).wait_send())

        return start, relay, wait, drain

    key_start, key_relay, key_wait, key_drain = window(kwin, "kw")
    value_start, value_relay, value_wait, value_drain = window(vwin, "vw")

    for kv in range(KVH):
        key_in(kv).wait()
        key_start(kv)

    def weight_rows(owner, zb, cr, sub):
        return pl.ds(owner * R + (cr + 2 * zb) * QUARTER + sub * SUB, SUB)

    def weight_start(s, sub):
        own = pl.ds((core + 2 * zbit) * QUARTER + sub * SUB, SUB)
        return remote(
            r["weight"].at[own],
            wfull.at[weight_rows(l, zbit, core, sub)],
            r["w_send"].at[0, s - 1, sub],
            r["w_recv"].at[0, L - s - 1, sub],
            local=lax.rem(l + s, L),
        )

    def weight_pass(s, sub, step):
        owner = lax.rem(l + s, L)
        zb = zbit if step < 3 else 1 - zbit
        part = wfull.at[weight_rows(owner, zb, core, sub)]
        return remote(
            part,
            part,
            r["w_send"].at[step, s - 1, sub],
            r["w_recv"].at[step, s - 1, sub],
            node=zpeer if step == 1 else partner,
        )

    def weight_relay(sub):
        for s in range(1, L):
            weight_start(L - s, sub).wait_recv()
            weight_pass(s, sub, 1).start()
            weight_pass(s, sub, 2).start()

    def weight_relay_again(sub):
        for s in range(1, L):
            weight_pass(s, sub, 1).wait_recv()
            weight_pass(s, sub, 3).start()

    for sub in range(4):
        for s in range(1, L):
            weight_start(s, sub).start()

    def hidden_swap(j):
        cols = pl.ds((2 * j + 1 - core) * GW, GW)
        return remote(
            r["hidden"].at[:, cols], hidp.at[j], r["h_send"].at[j], r["h_recv"].at[j], node=partner
        )

    for j in range(N // 2):
        hidden_swap(j).start()

    block = n

    def find(j, carry):
        first, start, length = carry
        size = r["lengths"][0, r["order"][0, j]]
        count = lax.div(size + (T - 1), T)
        inside = jnp.logical_and(first <= block, block < first + count)
        return (
            first + count,
            jnp.where(inside, first, start),
            jnp.where(inside, size, length),
        )

    zero = jnp.int32(0)
    _, doc_start, doc_length = lax.fori_loop(0, r["lengths"].shape[1], find, (zero, zero, zero))
    low = (doc_start - block + (DOCB - 1)) * T
    high = low + doc_length
    key_at = lax.broadcasted_iota(jnp.int32, (DOCB * T, T), 0)
    query_at = lax.broadcasted_iota(jnp.int32, (DOCB * T, T), 1) + (DOCB - 1) * T
    allowed = (key_at >= low) & (key_at < high) & (key_at <= query_at)
    r["bias"][...] = jnp.where(allowed, 0.0, masked_score)
    query_row = lax.broadcasted_iota(jnp.int32, (T, GC), 0) + (DOCB - 1) * T
    query_ok = query_row < high

    hidden_in.wait()
    weight_in.wait()
    for j in range(N // 2):
        cols = pl.ds(pl.multiple_of((2 * j + core) * GW, GW), GW)
        hid_t[pl.ds(j * GW, GW), 0:T] = hid[:, cols].T
    own_cols = pl.ds(pl.multiple_of(l * R, R), R)
    r["vacc"][...] = dot(hid[:, own_cols], wfull[pl.ds(pl.multiple_of(l * R, R), R)])
    for kv in range(KVH):
        query_in(kv).wait()
        grad_in(kv).wait()
        r["g"][kv] = jnp.where(query_ok, r["g"][kv].astype(F32), 0.0).astype(BF16)

    def backward(name):
        send, recv = r[name + "_send"], r[name + "_recv"]
        out, mid, comb = r[name + "_out"], r[name + "_mid"], r[name + "_comb"]
        near, third, own, keep = (r[name + e] for e in ("_near", "_third", "_own", "_keep"))
        to_third = jnp.logical_or(odd, has_far_prev)
        third_node = jnp.where(even, n - 3, n - 1)
        from_third = jnp.logical_or(even, has_far_next)

        def across(kv):
            return remote(out.at[kv, 0], mid.at[kv], send.at[0, kv], recv.at[0, kv], node=partner)

        def skip(kv):
            return remote(
                out.at[kv, 1], third.at[kv], send.at[1, kv], recv.at[1, kv], node=third_node
            )

        def back(kv):
            return remote(comb.at[kv], near.at[kv], send.at[2, kv], recv.at[2, kv], node=n - 2)

        def give(kv, acc):
            out[kv, 0] = acc[pl.ds((1 - core) * 2 * T, T)].astype(BF16)
            out[kv, 1] = acc[pl.ds(core * 2 * T, T)].astype(BF16)
            across(kv).start()
            pl.when(to_third)(lambda: skip(kv).start())
            keep[kv] = acc[rows(2)]
            own[kv] = acc[rows(0)]

        def combine(kv):
            across(kv).wait_recv()

            @pl.when(has_prev)
            def _():
                comb[kv] = (keep[kv] + mid[kv].astype(F32)).astype(BF16)
                back(kv).start()

        def total(kv):
            pl.when(from_third)(lambda: skip(kv).wait_recv())
            pl.when(has_next)(lambda: back(kv).wait_recv())
            return own[kv] + near[kv].astype(F32) + third[kv].astype(F32)

        def drain(kv):
            across(kv).wait_send()
            pl.when(to_third)(lambda: skip(kv).wait_send())
            pl.when(has_prev)(lambda: back(kv).wait_send())

        return give, combine, total, drain

    v_give, v_combine, v_total, v_drain = backward("v")
    k_give, k_combine, k_total, k_drain = backward("k")

    vl = r["vl"]

    def low_swap(kv):
        return remote(
            vl.at[kv, pl.ds(0, T)],
            vl.at[kv, pl.ds(T, T)],
            r["vl_send"].at[kv],
            r["vl_recv"].at[kv],
            node=partner,
        )

    def value_own(kv):
        vl[kv, 0:T] = v_total(kv).astype(BF16)
        low_swap(kv).start()

    wacc = r["wacc"]

    def y_copy(kv, s):
        return remote(
            r["ys"].at[kv, s - 1],
            r["yr"].at[kv, L - s - 1],
            r["y_send"].at[s - 1, kv],
            r["y_recv"].at[L - s - 1, kv],
            local=lax.rem(l + s, L),
        )

    def x_copy(kv):
        return remote(
            r["xs"].at[kv], r["xr"].at[kv], r["x_send"].at[kv], r["x_recv"].at[kv], node=xpeer
        )

    def z_copy(kv, s):
        return remote(
            r["zs"].at[kv, lax.rem(z + s, NZ)],
            r["zr"].at[kv, NZ - s - 1],
            r["z_send"].at[s - 1, kv],
            r["z_recv"].at[NZ - s - 1, kv],
            node=lax.rem(n + 4 * s, N),
        )

    def grad_terms(kv):
        low_swap(kv).wait_recv()
        both = vl[kv]
        for j in range(N // 2):
            part = dot(hid_t[pl.ds(j * GW, GW)], both)
            wacc[kv, j] = part.reshape(L, RO, C)
        for s in range(1, L):
            there = lax.rem(l + s, L)
            for j in range(N // 2):
                r["ys"][kv, s - 1, j] = wacc[kv, j, there].astype(BF16)
            y_copy(kv, s).start()

    def grad_y(kv):
        for s in range(1, L):
            y_copy(kv, L - s).wait_recv()

        def summed(j):
            total = wacc[kv, j, l]
            for s in range(1, L):
                total = total + r["yr"][kv, s - 1, j].astype(F32)
            return total

        for zz in range(NZ):
            r["xs"][kv, zz] = summed(2 * zz + 1 - xbit).astype(BF16)
        x_copy(kv).start()
        for zz in range(NZ):
            r["xk"][kv, zz] = summed(2 * zz + xbit)

    def grad_x(kv):
        x_copy(kv).wait_recv()
        for zz in range(NZ):
            total = r["xk"][kv, zz] + r["xr"][kv, zz].astype(F32)
            r["xk"][kv, zz] = total
            r["zs"][kv, zz] = total.astype(BF16)
        for s in range(1, NZ):
            z_copy(kv, s).start()

    def grad_z(kv):
        total = r["xk"][kv, z]
        for s in range(1, NZ):
            z_copy(kv, NZ - s).wait_recv()
        for s in range(1, NZ):
            total = total + r["zr"][kv, s - 1].astype(F32)
        r["dw"][kv] = total
        weight_grad_out(kv).start()

    def weight_grad_out(kv):
        return local_copy(
            r["dw"].at[kv], r["weight_grad"].at[:, pl.ds(kv * C, C)], r["out_sem"].at[0, kv]
        )

    def key_grad_out(kv):
        return local_copy(
            r["dk"].at[kv], r["key_grad"].at[:, pl.ds(kv * C, C)], r["out_sem"].at[1, kv]
        )

    def query_grad_out(kv):
        return local_copy(
            r["dq"].at[kv], r["query_grad"].at[:, pl.ds(kv * GC, GC)], r["out_sem"].at[2, kv]
        )

    def key_own(kv):
        r["dk"][kv] = k_total(kv).astype(BF16)
        key_grad_out(kv).start()

    probs, acc = r["probs"], r["acc"]

    def value_heads(kv, heads):
        keys = kwin[kv]
        for head in heads:
            cols = slice(head * C, (head + 1) * C)
            scores = dot_rows(keys, r["q"][kv, :, cols]) + r["bias"][...]
            top = jnp.max(scores, axis=0, keepdims=True)
            expd = jnp.exp2((scores - top) * (scale * LOG2E))
            low_probs = (expd * (1.0 / jnp.sum(expd, axis=0, keepdims=True))).astype(BF16)
            probs[kv * G + head] = low_probs
            part = dot(low_probs, r["g"][kv, :, cols])
            if head == 0:
                acc[...] = part
            else:
                acc[...] += part

    def key_heads(kv, heads):
        values = vwin[kv]
        turned = kwin[kv].T
        for head in heads:
            cols = slice(head * C, (head + 1) * C)
            prob_grad = dot_rows(values, r["g"][kv, :, cols])
            p = probs[kv * G + head].astype(F32)
            delta = jnp.sum(p * prob_grad, axis=0, keepdims=True)
            score_grad = (p * (prob_grad - delta) * scale).astype(BF16)
            r["dq"][kv, :, cols] = dot(turned, score_grad).T.astype(BF16)
            part = dot(score_grad, r["q"][kv, :, cols])
            if head == 0:
                acc[...] = part
            else:
                acc[...] += part

    half = G // 2
    first_heads, last_heads = tuple(range(half)), tuple(range(half, G))

    for j in range(N // 2):
        hidden_swap(j).wait_recv()
        hid_t[pl.ds(j * GW, GW), T : 2 * T] = hidp[j].T

    key_relay(0)

    def value_pass(kv, carry):
        pl.when(kv + 1 < KVH)(lambda: key_relay(kv + 1))
        key_wait(kv)
        weight_relay(kv)
        pl.when(kv >= 1)(lambda: weight_relay_again(kv - 1))
        value_heads(kv, first_heads)
        pl.when(kv >= 1)(lambda: v_combine(kv - 1))
        pl.when(kv >= 2)(lambda: value_own(kv - 2))
        value_heads(kv, last_heads)
        v_give(kv, acc)
        pl.when(kv >= 2)(lambda: grad_terms(kv - 2))
        return carry

    lax.fori_loop(0, KVH, value_pass, 0)

    last = KVH - 1
    weight_relay_again(3)
    value_own(last - 1)
    v_combine(last)

    for sub in range(4):
        for s in range(1, L):
            weight_pass(s, sub, 2).wait_recv()
            weight_pass(s, sub, 3).wait_recv()
    values = r["vacc"][...]
    for s in range(1, L):
        there = pl.multiple_of(lax.rem(l + s, L) * R, R)
        values = values + dot(hid[:, pl.ds(there, R)], wfull[pl.ds(there, R)])
    for kv in range(KVH):
        vwin[kv, rows(0)] = values[:, kv * C : (kv + 1) * C].astype(BF16)
        value_start(kv)

    grad_terms(last - 1)
    value_own(last)
    value_relay(0)

    def input_grad_out():
        return local_copy(r["dx"], r["input_grad"], r["in_sem"].at[2])

    own_low = jnp.concatenate([vl[kv, 0:T] for kv in range(KVH)], axis=1)
    step = 512

    def input_pass(i, carry):
        at = pl.multiple_of(i * step, step)
        r["dx"][:, pl.ds(at, step)] = dot_rows(own_low, wfull[pl.ds(at, step)]).astype(BF16)
        return carry

    lax.fori_loop(0, D // step, input_pass, 0)
    grad_terms(last)
    input_grad_out().start()

    def key_pass(kv, carry):
        pl.when(kv + 1 < KVH)(lambda: value_relay(kv + 1))
        value_wait(kv)
        key_heads(kv, first_heads)
        pl.when(kv >= 1)(lambda: k_combine(kv - 1))
        pl.when(kv >= 2)(lambda: key_own(kv - 2))
        key_heads(kv, last_heads)
        k_give(kv, acc)
        query_grad_out(kv).start()
        grad_y(kv)
        pl.when(kv >= 1)(lambda: grad_x(kv - 1))
        pl.when(kv >= 2)(lambda: grad_z(kv - 2))
        return carry

    lax.fori_loop(0, KVH, key_pass, 0)
    k_combine(last)
    grad_x(last)
    grad_z(last - 1)
    key_own(last - 1)
    key_own(last)
    grad_z(last)

    def drains(kv, carry):
        key_drain(kv)
        value_drain(kv)
        v_drain(kv)
        k_drain(kv)
        low_swap(kv).wait_send()
        for s in range(1, L):
            y_copy(kv, s).wait_send()
        x_copy(kv).wait_send()
        for s in range(1, NZ):
            z_copy(kv, s).wait_send()
        weight_grad_out(kv).wait()
        key_grad_out(kv).wait()
        query_grad_out(kv).wait()
        return carry

    lax.fori_loop(0, KVH, drains, 0)
    for sub in range(4):
        for s in range(1, L):
            weight_start(s, sub).wait_send()
            for step_id in (1, 2, 3):
                weight_pass(s, sub, step_id).wait_send()
    for j in range(N // 2):
        hidden_swap(j).wait_send()
    input_grad_out().wait()


def local(hidden, queries, saved_keys, grad_out, value_weight, doc_lengths, doc_order):
    N, L = lax.axis_size("node"), lax.axis_size("local")
    T, D = hidden.shape[1:]
    QW, KVW = queries.shape[2], saved_keys.shape[2]
    KVH = KVW // HD
    G = QW // KVW
    C = HD
    NZ, RO, GW, J = N // 4, D // (N * L), D // N, N // 2
    vmem = lambda *shape: lambda dtype: pltpu.VMEM(shape, dtype)
    dma = lambda *shape: pltpu.SemaphoreType.DMA(shape)
    scratch = dict(
        kwin=pltpu.VMEM((KVH, DOCB * T, C), BF16),
        vwin=pltpu.VMEM((KVH, DOCB * T, C), BF16),
        q=pltpu.VMEM((KVH, T, G * C), BF16),
        g=pltpu.VMEM((KVH, T, G * C), BF16),
        hid=pltpu.VMEM((T, D), BF16),
        hidp=pltpu.VMEM((J, T, GW), BF16),
        hid_t=pltpu.VMEM((J * GW, 2 * T), BF16),
        wfull=pltpu.VMEM((D, KVW), BF16),
        bias=pltpu.VMEM((DOCB * T, T), F32),
        vacc=pltpu.VMEM((T, KVW), F32),
        probs=pltpu.VMEM((KVH * G, DOCB * T, T), BF16),
        acc=pltpu.VMEM((DOCB * T, C), F32),
        vl=pltpu.VMEM((KVH, 2 * T, C), BF16),
        wacc=pltpu.VMEM((KVH, J, L, RO, C), F32),
        ys=pltpu.VMEM((KVH, L - 1, J, RO, C), BF16),
        yr=pltpu.VMEM((KVH, L - 1, J, RO, C), BF16),
        xs=pltpu.VMEM((KVH, NZ, RO, C), BF16),
        xr=pltpu.VMEM((KVH, NZ, RO, C), BF16),
        xk=pltpu.VMEM((KVH, NZ, RO, C), F32),
        zs=pltpu.VMEM((KVH, NZ, RO, C), BF16),
        zr=pltpu.VMEM((KVH, NZ - 1, RO, C), BF16),
        dw=pltpu.VMEM((KVH, RO, C), F32),
        dk=pltpu.VMEM((KVH, T, C), BF16),
        dq=pltpu.VMEM((KVH, T, G * C), BF16),
        dx=pltpu.VMEM((T, D), BF16),
        key_in_sem=dma(KVH),
        query_in_sem=dma(KVH),
        grad_in_sem=dma(KVH),
        in_sem=dma(3),
        out_sem=dma(3, KVH),
        w_send=dma(4, L - 1, 4),
        w_recv=dma(4, L - 1, 4),
        h_send=dma(J),
        h_recv=dma(J),
        vl_send=dma(KVH),
        vl_recv=dma(KVH),
        y_send=dma(L - 1, KVH),
        y_recv=dma(L - 1, KVH),
        x_send=dma(KVH),
        x_recv=dma(KVH),
        z_send=dma(NZ - 1, KVH),
        z_recv=dma(NZ - 1, KVH),
    )
    for name in ("kw", "vw", "v", "k"):
        scratch[name + "_send"] = dma(3, KVH)
        scratch[name + "_recv"] = dma(3, KVH)
    for name in ("v", "k"):
        scratch[name + "_out"] = pltpu.VMEM((KVH, 2, T, C), BF16)
        for extra in ("_mid", "_comb", "_near", "_third"):
            scratch[name + extra] = pltpu.VMEM((KVH, T, C), BF16)
        for extra in ("_own", "_keep"):
            scratch[name + extra] = pltpu.VMEM((KVH, T, C), F32)
    args = ("lengths", "order", "hidden", "queries", "keys", "grads", "weight")
    outs = ("query_grad", "key_grad", "input_grad", "weight_grad")
    sizes = dict(N=N, L=L, T=T, D=D, KVH=KVH, G=G, names=args + outs + tuple(scratch))
    smem = pl.BlockSpec(memory_space=pltpu.SMEM)
    anywhere = pl.BlockSpec(memory_space=pl.ANY)
    query_grad, key_grad, input_grad, weight_grad = pl.pallas_call(
        functools.partial(kernel, sizes),
        out_shape=[
            jax.ShapeDtypeStruct((T, QW), BF16),
            jax.ShapeDtypeStruct((T, KVW), BF16),
            jax.ShapeDtypeStruct((T, D), BF16),
            jax.ShapeDtypeStruct((RO, KVW), F32),
        ],
        in_specs=[smem, smem] + [anywhere] * 5,
        out_specs=[anywhere] * 4,
        scratch_shapes=list(scratch.values()),
        compiler_params=pltpu.CompilerParams(
            collective_id=0, has_side_effects=True, vmem_limit_bytes=60 * 2**20
        ),
        name="attention_grads",
    )(
        doc_lengths,
        doc_order,
        hidden[0],
        queries[0],
        saved_keys[0],
        grad_out[0],
        value_weight,
    )
    return query_grad[None], key_grad[None], input_grad[None], weight_grad


def solution(mesh):
    tokens = P("local", "node", None)
    return jax.shard_map(
        local,
        mesh=mesh,
        in_specs=(tokens,) * 4 + (P("local", None),) * 3,
        out_specs=(tokens,) * 3 + (P(("node", "local"), None),),
        check_vma=False,
    )
```

```python
import functools

import jax
import jax.numpy as jnp
from jax import lax
from jax.experimental import pallas as pl
from jax.experimental.pallas import tpu as pltpu
from jax.sharding import PartitionSpec as P

HD = 128
DOCB = 4
BF16 = jnp.bfloat16
F32 = jnp.float32
LOG2E = 1.4426950408889634
MESH = pl.DeviceIdType.MESH

masked_score = -1e30
X_FIRST = ()

ROWS_BY_ROWS = (((1,), (1,)), ((), ()))


def dot(a, b):
    return jnp.dot(a, b, preferred_element_type=F32)


def dot_rows(a, b):
    return lax.dot_general(a, b, ROWS_BY_ROWS, preferred_element_type=F32)


def remote(src, dst, send_sem, recv_sem, **where):
    return pltpu.make_async_remote_copy(
        src_ref=src,
        dst_ref=dst,
        send_sem=send_sem,
        recv_sem=recv_sem,
        device_id=where,
        device_id_type=MESH,
    )


def scoped(name):
    def wrap(function):
        @functools.wraps(function)
        def inner(*args):
            with jax.named_scope(name):
                return function(*args)

        return inner

    return wrap


def kernel(sizes, *refs):
    N, L, T, D, KVH, G = (sizes[k] for k in ("N", "L", "T", "D", "KVH", "G"))
    names = sizes["names"]
    r = dict(zip(names, refs))
    C = HD
    NZ = N // 4
    RO = D // (N * L)
    GW = D // N
    R = D // L
    QUARTER, SUB = R // 4, R // 16
    GC = G * C
    scale = HD ** (-0.5)

    n = lax.axis_index("node")
    l = lax.axis_index("local")
    core = lax.rem(n, 2)
    even, odd = core == 0, core == 1
    partner = n + 1 - 2 * core
    xbit = lax.rem(lax.div(n, 2), 2)
    xpeer = n + 2 - 4 * xbit
    z = lax.div(n, 4)
    zbit = lax.rem(z, 2)
    zpeer = n + 4 - 8 * zbit
    has_next, has_prev = n + 2 < N, n >= 2
    has_far_next, has_far_prev = n + 3 < N, n >= 3

    kwin, vwin = r["kwin"], r["vwin"]
    hid, hidp, hid_t, wfull = r["hid"], r["hidp"], r["hid_t"], r["wfull"]

    def rows(offset):
        return pl.ds((DOCB - 1 - offset) * T, T)

    for offset in range(1, DOCB):

        @pl.when(n < offset)
        def _():
            for win in (kwin, vwin):
                for kv in range(KVH):
                    win[kv, rows(offset)] = jnp.zeros((T, C), BF16)

    for name in ("v", "k"):

        @pl.when(n + 2 >= N)
        def _():
            r[name + "_near"][...] = jnp.zeros((KVH, T, C), BF16)

        @pl.when(jnp.logical_and(odd, n + 3 >= N))
        def _():
            r[name + "_third"][...] = jnp.zeros((KVH, T, C), BF16)

    def local_copy(src, dst, sem):
        return pltpu.make_async_copy(src, dst, sem)

    def key_in(kv):
        return local_copy(
            r["keys"].at[:, pl.ds(kv * C, C)], kwin.at[kv, rows(0)], r["key_in_sem"].at[kv]
        )

    def query_in(kv):
        cols = pl.ds(kv * GC, GC)
        return local_copy(r["queries"].at[:, cols], r["q"].at[kv], r["query_in_sem"].at[kv])

    def grad_in(kv):
        cols = pl.ds(kv * GC, GC)
        return local_copy(r["grads"].at[:, cols], r["g"].at[kv], r["grad_in_sem"].at[kv])

    hidden_in = local_copy(r["hidden"], hid, r["in_sem"].at[0])
    weight_in = local_copy(r["weight"], wfull.at[pl.ds(l * R, R)], r["in_sem"].at[1])
    for kv in range(KVH):
        key_in(kv).start()
    hidden_in.start()
    weight_in.start()
    for kv in range(KVH):
        query_in(kv).start()
        grad_in(kv).start()

    barrier = pltpu.get_barrier_semaphore()

    def greet(**where):
        pl.semaphore_signal(barrier, inc=1, device_id=where, device_id_type=MESH)

    greet(node=partner)
    for there, who in (
        (has_next, n + 2),
        (has_prev, n - 2),
        (jnp.logical_and(odd, has_far_next), n + 3),
        (jnp.logical_and(even, has_far_prev), n - 3),
    ):

        @pl.when(there)
        def _():
            greet(node=who)

    for s in range(1, L):
        greet(local=lax.rem(l + s, L))
    for s in range(1, NZ):
        greet(node=lax.rem(n + 4 * s, N))
    as_int = lambda b: jnp.where(b, 1, 0)
    expected = (
        1
        + as_int(has_next)
        + as_int(has_prev)
        + core * as_int(has_far_next)
        + (1 - core) * as_int(has_far_prev)
        + (L - 1)
        + (NZ - 1)
    )
    with jax.named_scope("entry"):
        pl.semaphore_wait(barrier, expected)

    def window(win, name):
        send, recv = r[name + "_send"], r[name + "_recv"]

        def ahead(kv):
            return remote(
                win.at[kv, rows(0)], win.at[kv, rows(2)], send.at[0, kv], recv.at[1, kv], node=n + 2
            )

        def beside(kv):
            return remote(
                win.at[kv, rows(0)], win.at[kv, rows(1)], send.at[1, kv], recv.at[0, kv], node=n + 1
            )

        def far(kv):
            return remote(
                win.at[kv, rows(0)], win.at[kv, rows(3)], send.at[1, kv], recv.at[2, kv], node=n + 3
            )

        def relay_even(kv):
            return remote(
                win.at[kv, rows(2)], win.at[kv, rows(3)], send.at[2, kv], recv.at[2, kv], node=n + 1
            )

        def relay_odd(kv):
            return remote(
                win.at[kv, rows(2)], win.at[kv, rows(1)], send.at[2, kv], recv.at[0, kv], node=n - 1
            )

        far_there = jnp.logical_and(odd, has_far_next)
        relay_e = jnp.logical_and(even, has_prev)
        relay_o = jnp.logical_and(odd, has_prev)

        @scoped(name + "_start")
        def start(kv):
            pl.when(has_next)(lambda: ahead(kv).start())
            pl.when(far_there)(lambda: far(kv).start())
            pl.when(even)(lambda: beside(kv).start())

        @scoped(name + "_relay")
        def relay(kv):
            @pl.when(has_prev)
            def _():
                ahead(kv).wait_recv()

            pl.when(relay_e)(lambda: relay_even(kv).start())
            pl.when(relay_o)(lambda: relay_odd(kv).start())

        @scoped(name + "_wait")
        def wait(kv):
            pl.when(jnp.logical_or(odd, has_prev))(lambda: beside(kv).wait_recv())
            pl.when(has_far_prev)(lambda: far(kv).wait_recv())

        def drain(kv):
            pl.when(has_next)(lambda: ahead(kv).wait_send())
            pl.when(jnp.logical_or(even, has_far_next))(lambda: far(kv).wait_send())
            pl.when(has_prev)(lambda: relay_even(kv).wait_send())

        return start, relay, wait, drain

    key_start, key_relay, key_wait, key_drain = window(kwin, "kw")
    value_start, value_relay, value_wait, value_drain = window(vwin, "vw")

    for kv in range(2):
        key_in(kv).wait()
        key_start(kv)

    def weight_part(owner, zb, xb, sub):
        return pl.ds(owner * R + (zb * 2 + xb) * QUARTER + (core * 2 + sub) * SUB, SUB)

    def weight_class(owner, index):
        if index < 2:
            return weight_part(owner, zbit, xbit, index)
        return weight_part(owner, 1 - zbit, 1 - xbit, index - 2)

    def weight_start(s, index):
        return remote(
            r["weight"].at[weight_class(0, index)],
            wfull.at[weight_class(l, index)],
            r["w_send"].at[0, s - 1, index],
            r["w_recv"].at[0, L - s - 1, index],
            local=lax.rem(l + s, L),
        )

    def weight_pass(s, index, kind):
        owner = lax.rem(l + s, L)
        if kind <= 3:
            rows_at = weight_class(owner, index)
        elif kind == 4:
            rows_at = weight_part(owner, 1 - zbit, xbit, index)
        else:
            rows_at = weight_part(owner, zbit, 1 - xbit, index)
        part = wfull.at[rows_at]
        return remote(
            part,
            part,
            r["w_send"].at[kind, s - 1, index],
            r["w_recv"].at[kind, s - 1, index],
            node={1: zpeer, 2: xpeer}.get(kind, partner),
        )

    @scoped("weight_relay")
    def weight_relay(index):
        for s in range(1, L):
            weight_start(L - s, index).wait_recv()
            if index < 2:
                weight_pass(s, index, 1).start()
                weight_pass(s, index, 2).start()
            weight_pass(s, index, 3).start()

    @scoped("weight_again")
    def weight_relay_again(sub):
        for s in range(1, L):
            weight_pass(s, sub, 1).wait_recv()
            weight_pass(s, sub, 4).start()
            weight_pass(s, sub, 2).wait_recv()
            weight_pass(s, sub, 5).start()

    weight_kinds = [(k, i) for k in (3, 1, 2, 4, 5) for i in range(4) if k == 3 or i < 2]

    for sub in range(4):
        for s in range(1, L):
            weight_start(s, sub).start()

    def hidden_swap(j):
        cols = pl.ds((2 * j + 1 - core) * GW, GW)
        return remote(
            r["hidden"].at[:, cols], hidp.at[j], r["h_send"].at[j], r["h_recv"].at[j], node=partner
        )

    block = n

    def find(j, carry):
        first, start, length = carry
        size = r["lengths"][0, r["order"][0, j]]
        count = lax.div(size + (T - 1), T)
        inside = jnp.logical_and(first <= block, block < first + count)
        return (
            first + count,
            jnp.where(inside, first, start),
            jnp.where(inside, size, length),
        )

    zero = jnp.int32(0)
    _, doc_start, doc_length = lax.fori_loop(0, r["lengths"].shape[1], find, (zero, zero, zero))
    low = (doc_start - block + (DOCB - 1)) * T
    high = low + doc_length
    key_at = lax.broadcasted_iota(jnp.int32, (DOCB * T, T), 0)
    query_at = lax.broadcasted_iota(jnp.int32, (DOCB * T, T), 1) + (DOCB - 1) * T
    allowed = (key_at >= low) & (key_at < high) & (key_at <= query_at)
    r["bias"][...] = jnp.where(allowed, 0.0, masked_score)
    query_row = lax.broadcasted_iota(jnp.int32, (T, GC), 0) + (DOCB - 1) * T
    query_ok = query_row < high

    with jax.named_scope("hid_in"):
        hidden_in.wait()
    weight_in.wait()
    with jax.named_scope("turn_hid"):
      for j in range(N // 2):
        cols = pl.ds(pl.multiple_of((2 * j + core) * GW, GW), GW)
        hid_t[pl.ds(j * GW, GW), 0:T] = hid[:, cols].T
    own_cols = pl.ds(pl.multiple_of(l * R, R), R)
    with jax.named_scope("half_values"):
        r["vacc"][...] = dot(hid[:, own_cols], wfull[pl.ds(pl.multiple_of(l * R, R), R)])
    for kv in range(KVH):
        query_in(kv).wait()
        grad_in(kv).wait()
    with jax.named_scope("mask_g"):
      for kv in range(KVH):
        r["g"][kv] = jnp.where(query_ok, r["g"][kv].astype(F32), 0.0).astype(BF16)

    def backward(name):
        send, recv = r[name + "_send"], r[name + "_recv"]
        out, mid, comb = r[name + "_out"], r[name + "_mid"], r[name + "_comb"]
        near, third, own, keep = (r[name + e] for e in ("_near", "_third", "_own", "_keep"))
        to_third = jnp.logical_or(odd, has_far_prev)
        third_node = jnp.where(even, n - 3, n - 1)
        from_third = jnp.logical_or(even, has_far_next)

        def across(kv):
            return remote(out.at[kv, 0], mid.at[kv], send.at[0, kv], recv.at[0, kv], node=partner)

        def skip(kv):
            return remote(
                out.at[kv, 1], third.at[kv], send.at[1, kv], recv.at[1, kv], node=third_node
            )

        def back(kv):
            return remote(comb.at[kv], near.at[kv], send.at[2, kv], recv.at[2, kv], node=n - 2)

        @scoped(name + "_give")
        def give(kv, acc):
            out[kv, 0] = acc[pl.ds((1 - core) * 2 * T, T)].astype(BF16)
            out[kv, 1] = acc[pl.ds(core * 2 * T, T)].astype(BF16)
            across(kv).start()
            pl.when(to_third)(lambda: skip(kv).start())
            keep[kv] = acc[rows(2)]
            own[kv] = acc[rows(0)]

        @scoped(name + "_combine")
        def combine(kv):
            across(kv).wait_recv()

            @pl.when(has_prev)
            def _():
                comb[kv] = (keep[kv] + mid[kv].astype(F32)).astype(BF16)
                back(kv).start()

        def total(kv):
            pl.when(from_third)(lambda: skip(kv).wait_recv())
            pl.when(has_next)(lambda: back(kv).wait_recv())
            return own[kv] + near[kv].astype(F32) + third[kv].astype(F32)

        def drain(kv):
            across(kv).wait_send()
            pl.when(to_third)(lambda: skip(kv).wait_send())
            pl.when(has_prev)(lambda: back(kv).wait_send())

        return give, combine, total, drain

    v_give, v_combine, v_total, v_drain = backward("v")
    k_give, k_combine, k_total, k_drain = backward("k")

    vl = r["vl"]

    def low_swap(kv):
        return remote(
            vl.at[kv, pl.ds(0, T)],
            vl.at[kv, pl.ds(T, T)],
            r["vl_send"].at[kv],
            r["vl_recv"].at[kv],
            node=partner,
        )

    @scoped("value_own")
    def value_own(kv):
        vl[kv, 0:T] = v_total(kv).astype(BF16)
        low_swap(kv).start()

    wacc, xk = r["wacc"], r["xk"]

    def y_copy(kv, s, first):
        size = N // 2 if first else NZ
        return remote(
            r["ys"].at[kv, s - 1, pl.ds(0, size)],
            r["yr"].at[kv, L - s - 1, pl.ds(0, size)],
            r["y_send"].at[s - 1, kv],
            r["y_recv"].at[L - s - 1, kv],
            local=lax.rem(l + s, L),
        )

    def x_copy(kv, first):
        size = L if first else 1
        return remote(
            r["xs"].at[kv, pl.ds(0, size)],
            r["xr"].at[kv, pl.ds(0, size)],
            r["x_send"].at[kv],
            r["x_recv"].at[kv],
            node=xpeer,
        )

    def z_copy(kv, s):
        return remote(
            r["zs"].at[kv, lax.rem(z + s, NZ)],
            r["zr"].at[kv, NZ - s - 1],
            r["z_send"].at[s - 1, kv],
            r["z_recv"].at[NZ - s - 1, kv],
            node=lax.rem(n + 4 * s, N),
        )

    x_first = lambda kv: kv in X_FIRST

    @scoped("terms")
    def grad_terms(kv):
        low_swap(kv).wait_recv()
        both = vl[kv]
        for j in range(N // 2):
            part = dot(hid_t[pl.ds(j * GW, GW)], both)
            wacc[kv, j] = part.reshape(L, RO, C)
        if x_first(kv):
            for zz in range(NZ):
                for there in range(L):
                    r["xs"][kv, there, zz] = wacc[kv, 2 * zz + 1 - xbit, there].astype(BF16)
            x_copy(kv, True).start()
            return
        for s in range(1, L):
            there = lax.rem(l + s, L)
            for j in range(N // 2):
                r["ys"][kv, s - 1, j] = wacc[kv, j, there].astype(BF16)
            y_copy(kv, s, True).start()

    @scoped("second")
    def grad_second(kv):
        if x_first(kv):
            x_copy(kv, True).wait_recv()

            def joined(zz, there):
                return wacc[kv, 2 * zz + xbit, there] + r["xr"][kv, there, zz].astype(F32)

            for s in range(1, L):
                there = lax.rem(l + s, L)
                for zz in range(NZ):
                    r["ys"][kv, s - 1, zz] = joined(zz, there).astype(BF16)
                y_copy(kv, s, False).start()
            for zz in range(NZ):
                xk[kv, zz] = joined(zz, l)
            return
        for s in range(1, L):
            y_copy(kv, L - s, True).wait_recv()

        def summed(j):
            total = wacc[kv, j, l]
            for s in range(1, L):
                total = total + r["yr"][kv, s - 1, j].astype(F32)
            return total

        for zz in range(NZ):
            r["xs"][kv, 0, zz] = summed(2 * zz + 1 - xbit).astype(BF16)
        x_copy(kv, False).start()
        for zz in range(NZ):
            xk[kv, zz] = summed(2 * zz + xbit)

    @scoped("third")
    def grad_third(kv):
        if x_first(kv):
            for s in range(1, L):
                y_copy(kv, L - s, False).wait_recv()
        else:
            x_copy(kv, False).wait_recv()
        for zz in range(NZ):
            total = xk[kv, zz]
            if x_first(kv):
                for s in range(1, L):
                    total = total + r["yr"][kv, s - 1, zz].astype(F32)
            else:
                total = total + r["xr"][kv, 0, zz].astype(F32)
            xk[kv, zz] = total
            r["zs"][kv, zz] = total.astype(BF16)
        for s in range(1, NZ):
            z_copy(kv, s).start()

    @scoped("final")
    def grad_final(kv):
        total = xk[kv, z]
        for s in range(1, NZ):
            z_copy(kv, NZ - s).wait_recv()
        for s in range(1, NZ):
            total = total + r["zr"][kv, s - 1].astype(F32)
        r["dw"][kv] = total
        weight_grad_out(kv).start()

    def weight_grad_out(kv):
        return local_copy(
            r["dw"].at[kv], r["weight_grad"].at[:, pl.ds(kv * C, C)], r["out_sem"].at[0, kv]
        )

    def key_grad_out(kv):
        return local_copy(
            r["dk"].at[kv], r["key_grad"].at[:, pl.ds(kv * C, C)], r["out_sem"].at[1, kv]
        )

    def query_grad_out(kv):
        return local_copy(
            r["dq"].at[kv], r["query_grad"].at[:, pl.ds(kv * GC, GC)], r["out_sem"].at[2, kv]
        )

    @scoped("key_own")
    def key_own(kv):
        r["dk"][kv] = k_total(kv).astype(BF16)
        key_grad_out(kv).start()

    probs, acc = r["probs"], r["acc"]

    @scoped("value_heads")
    def value_heads(kv, heads):
        keys = kwin[kv]
        for head in heads:
            cols = slice(head * C, (head + 1) * C)
            scores = dot_rows(keys, r["q"][kv, :, cols]) + r["bias"][...]
            top = jnp.max(scores, axis=0, keepdims=True)
            expd = jnp.exp2((scores - top) * (scale * LOG2E))
            low_probs = (expd * (1.0 / jnp.sum(expd, axis=0, keepdims=True))).astype(BF16)
            probs[kv * G + head] = low_probs
            part = dot(low_probs, r["g"][kv, :, cols])
            if head == 0:
                acc[...] = part
            else:
                acc[...] += part

    @scoped("key_heads")
    def key_heads(kv, heads):
        values = vwin[kv]
        turned = kwin[kv].T
        for head in heads:
            cols = slice(head * C, (head + 1) * C)
            prob_grad = dot_rows(values, r["g"][kv, :, cols])
            p = probs[kv * G + head].astype(F32)
            delta = jnp.sum(p * prob_grad, axis=0, keepdims=True)
            score_grad = (p * (prob_grad - delta) * scale).astype(BF16)
            r["dq"][kv, :, cols] = dot(turned, score_grad).T.astype(BF16)
            part = dot(score_grad, r["q"][kv, :, cols])
            if head == 0:
                acc[...] = part
            else:
                acc[...] += part

    half = G // 2
    first_heads, last_heads = tuple(range(half)), tuple(range(half, G))
    last = KVH - 1

    def at(kv, plan):
        for when_kv in sorted({k for k, *_ in plan}):

            @pl.when(kv == when_kv)
            def _():
                for k, task, *args in plan:
                    if k == when_kv:
                        task(*args)

    @scoped("partner_hid")
    def partner_hidden():
        for j in range(N // 2):
            hidden_swap(j).wait_recv()
            hid_t[pl.ds(j * GW, GW), T : 2 * T] = hidp[j].T

    def more_keys(kv):
        key_in(kv).wait()
        key_start(kv)

    key_relay(0)
    for j in range(N // 2):
        hidden_swap(j).start()

    value_start_plan = [(kv, more_keys, kv + 2) for kv in range(KVH - 2)]
    value_mid_plan = (
        [(kv, key_relay, kv + 1) for kv in range(KVH - 1)]
        + [(kv, weight_relay, kv) for kv in range(KVH)]
        + [(kv, v_combine, kv - 1) for kv in range(1, KVH)]
        + [(1, partner_hidden)]
        + [(2, weight_relay_again, 0), (3, weight_relay_again, 1)]
        + [(3, grad_terms, 0)]
    )
    value_end_plan = [(kv, value_own, kv - 2) for kv in range(2, KVH)]

    def value_pass(kv, carry):
        key_wait(kv)
        at(kv, value_start_plan)
        value_heads(kv, first_heads)
        at(kv, value_mid_plan)
        value_heads(kv, last_heads)
        v_give(kv, acc)
        at(kv, value_end_plan)
        return carry

    lax.fori_loop(0, KVH, value_pass, 0)

    v_combine(last)
    grad_terms(1)
    value_own(2)

    with jax.named_scope("weight_wait"):
        for s in range(1, L):
            for kind, index in weight_kinds:
                if kind >= 3:
                    weight_pass(s, index, kind).wait_recv()
    with jax.named_scope("rest_values"):
        values = r["vacc"][...]
        for s in range(1, L):
            there = pl.multiple_of(lax.rem(l + s, L) * R, R)
            values = values + dot(hid[:, pl.ds(there, R)], wfull[pl.ds(there, R)])
        for kv in range(KVH):
            vwin[kv, rows(0)] = values[:, kv * C : (kv + 1) * C].astype(BF16)
    for kv in range(KVH):
        value_start(kv)
    grad_terms(2)
    value_own(last)

    def input_grad_out():
        return local_copy(r["dx"], r["input_grad"], r["in_sem"].at[2])

    step = D // 8

    def input_passes(low, high):
        own_low = jnp.concatenate([vl[kv, 0:T] for kv in range(KVH)], axis=1)

        def input_pass(i, carry):
            at = pl.multiple_of(i * step, step)
            r["dx"][:, pl.ds(at, step)] = dot_rows(own_low, wfull[pl.ds(at, step)]).astype(BF16)
            return carry

        with jax.named_scope("input_grad"):
            lax.fori_loop(low, high, input_pass, 0)

    input_passes(0, 4)
    grad_terms(last)
    value_relay(0)

    key_mid_plan = (
        [(kv, value_relay, kv + 1) for kv in range(KVH - 1)]
        + [(kv, k_combine, kv - 1) for kv in range(1, KVH)]
        + [(0, grad_second, 0), (1, grad_second, 1), (2, grad_second, 2), (3, grad_second, 3)]
    )
    key_end_plan = [(kv, key_own, kv - 2) for kv in range(2, KVH)] + [
        (1, grad_third, 0),
        (2, grad_third, 1),
        (2, grad_final, 0),
        (3, grad_third, 2),
        (3, grad_final, 1),
    ]

    def key_pass(kv, carry):
        value_wait(kv)
        key_heads(kv, first_heads)
        at(kv, key_mid_plan)
        key_heads(kv, last_heads)
        k_give(kv, acc)
        query_grad_out(kv).start()
        at(kv, key_end_plan)
        return carry

    lax.fori_loop(0, KVH, key_pass, 0)
    input_passes(4, 8)
    input_grad_out().start()
    k_combine(last)
    grad_third(last)
    key_own(last - 1)
    grad_final(last - 1)
    key_own(last)
    grad_final(last)

    def drains(kv, carry):
        key_drain(kv)
        value_drain(kv)
        v_drain(kv)
        k_drain(kv)
        low_swap(kv).wait_send()
        for s in range(1, NZ):
            z_copy(kv, s).wait_send()
        weight_grad_out(kv).wait()
        key_grad_out(kv).wait()
        query_grad_out(kv).wait()
        return carry

    with jax.named_scope("drains"):
        lax.fori_loop(0, KVH, drains, 0)
    for s in range(1, L):
        for index in range(4):
            weight_start(s, index).wait_send()
        for kind, index in weight_kinds:
            weight_pass(s, index, kind).wait_send()
    for kv in range(KVH):
        for s in range(1, L):
            y_copy(kv, s, not x_first(kv)).wait_send()
        x_copy(kv, x_first(kv)).wait_send()
    for j in range(N // 2):
        hidden_swap(j).wait_send()
    input_grad_out().wait()


def local(hidden, queries, saved_keys, grad_out, value_weight, doc_lengths, doc_order):
    N, L = lax.axis_size("node"), lax.axis_size("local")
    T, D = hidden.shape[1:]
    QW, KVW = queries.shape[2], saved_keys.shape[2]
    KVH = KVW // HD
    G = QW // KVW
    C = HD
    NZ, RO, GW, J = N // 4, D // (N * L), D // N, N // 2
    vmem = lambda *shape: lambda dtype: pltpu.VMEM(shape, dtype)
    dma = lambda *shape: pltpu.SemaphoreType.DMA(shape)
    scratch = dict(
        kwin=pltpu.VMEM((KVH, DOCB * T, C), BF16),
        vwin=pltpu.VMEM((KVH, DOCB * T, C), BF16),
        q=pltpu.VMEM((KVH, T, G * C), BF16),
        g=pltpu.VMEM((KVH, T, G * C), BF16),
        hid=pltpu.VMEM((T, D), BF16),
        hidp=pltpu.VMEM((J, T, GW), BF16),
        hid_t=pltpu.VMEM((J * GW, 2 * T), BF16),
        wfull=pltpu.VMEM((D, KVW), BF16),
        bias=pltpu.VMEM((DOCB * T, T), F32),
        vacc=pltpu.VMEM((T, KVW), F32),
        probs=pltpu.VMEM((KVH * G, DOCB * T, T), BF16),
        acc=pltpu.VMEM((DOCB * T, C), F32),
        vl=pltpu.VMEM((KVH, 2 * T, C), BF16),
        wacc=pltpu.VMEM((KVH, J, L, RO, C), F32),
        ys=pltpu.VMEM((KVH, L - 1, J, RO, C), BF16),
        yr=pltpu.VMEM((KVH, L - 1, J, RO, C), BF16),
        xs=pltpu.VMEM((KVH, L, NZ, RO, C), BF16),
        xr=pltpu.VMEM((KVH, L, NZ, RO, C), BF16),
        xk=pltpu.VMEM((KVH, NZ, RO, C), F32),
        zs=pltpu.VMEM((KVH, NZ, RO, C), BF16),
        zr=pltpu.VMEM((KVH, NZ - 1, RO, C), BF16),
        dw=pltpu.VMEM((KVH, RO, C), F32),
        dk=pltpu.VMEM((KVH, T, C), BF16),
        dq=pltpu.VMEM((KVH, T, G * C), BF16),
        dx=pltpu.VMEM((T, D), BF16),
        key_in_sem=dma(KVH),
        query_in_sem=dma(KVH),
        grad_in_sem=dma(KVH),
        in_sem=dma(3),
        out_sem=dma(3, KVH),
        w_send=dma(6, L - 1, 4),
        w_recv=dma(6, L - 1, 4),
        h_send=dma(J),
        h_recv=dma(J),
        vl_send=dma(KVH),
        vl_recv=dma(KVH),
        y_send=dma(L - 1, KVH),
        y_recv=dma(L - 1, KVH),
        x_send=dma(KVH),
        x_recv=dma(KVH),
        z_send=dma(NZ - 1, KVH),
        z_recv=dma(NZ - 1, KVH),
    )
    for name in ("kw", "vw", "v", "k"):
        scratch[name + "_send"] = dma(3, KVH)
        scratch[name + "_recv"] = dma(3, KVH)
    for name in ("v", "k"):
        scratch[name + "_out"] = pltpu.VMEM((KVH, 2, T, C), BF16)
        for extra in ("_mid", "_comb", "_near", "_third"):
            scratch[name + extra] = pltpu.VMEM((KVH, T, C), BF16)
        for extra in ("_own", "_keep"):
            scratch[name + extra] = pltpu.VMEM((KVH, T, C), F32)
    args = ("lengths", "order", "hidden", "queries", "keys", "grads", "weight")
    outs = ("query_grad", "key_grad", "input_grad", "weight_grad")
    sizes = dict(N=N, L=L, T=T, D=D, KVH=KVH, G=G, names=args + outs + tuple(scratch))
    smem = pl.BlockSpec(memory_space=pltpu.SMEM)
    anywhere = pl.BlockSpec(memory_space=pl.ANY)
    query_grad, key_grad, input_grad, weight_grad = pl.pallas_call(
        functools.partial(kernel, sizes),
        out_shape=[
            jax.ShapeDtypeStruct((T, QW), BF16),
            jax.ShapeDtypeStruct((T, KVW), BF16),
            jax.ShapeDtypeStruct((T, D), BF16),
            jax.ShapeDtypeStruct((RO, KVW), F32),
        ],
        in_specs=[smem, smem] + [anywhere] * 5,
        out_specs=[anywhere] * 4,
        scratch_shapes=list(scratch.values()),
        compiler_params=pltpu.CompilerParams(
            collective_id=0, has_side_effects=True, vmem_limit_bytes=60 * 2**20
        ),
        name="attention_grads",
    )(
        doc_lengths,
        doc_order,
        hidden[0],
        queries[0],
        saved_keys[0],
        grad_out[0],
        value_weight,
    )
    query_grad, key_grad, input_grad, weight_grad = results(
        query_grad, key_grad, input_grad, weight_grad
    )
    return query_grad[None], key_grad[None], input_grad[None], weight_grad


def results_kernel(count, *refs):
    sources, outs, held, sems = refs[:count], refs[count : 2 * count], refs[2 * count : -1], refs[-1]
    ins = [pltpu.make_async_copy(a, b, sems.at[0, i]) for i, (a, b) in enumerate(zip(sources, held))]
    backs = [pltpu.make_async_copy(b, c, sems.at[1, i]) for i, (b, c) in enumerate(zip(held, outs))]
    for copy in ins:
        copy.start()
    for copy, back in zip(ins, backs):
        copy.wait()
        back.start()
    for back in backs:
        back.wait()


def results(*arrays):
    anywhere = pl.BlockSpec(memory_space=pl.ANY)
    return pl.pallas_call(
        functools.partial(results_kernel, len(arrays)),
        out_shape=[jax.ShapeDtypeStruct(a.shape, a.dtype) for a in arrays],
        in_specs=[anywhere] * len(arrays),
        out_specs=[anywhere] * len(arrays),
        scratch_shapes=[pltpu.VMEM(a.shape, a.dtype) for a in arrays]
        + [pltpu.SemaphoreType.DMA((2, len(arrays)))],
        name="results",
    )(*arrays)


def solution(mesh):
    tokens = P("local", "node", None)
    return jax.shard_map(
        local,
        mesh=mesh,
        in_specs=(tokens,) * 4 + (P("local", None),) * 3,
        out_specs=(tokens,) * 3 + (P(("node", "local"), None),),
        check_vma=False,
    )
```

```python
import functools

import jax
import jax.numpy as jnp
from jax import lax
from jax.experimental import pallas as pl
from jax.experimental.pallas import tpu as pltpu
from jax.sharding import PartitionSpec as P

HD = 128
DOCB = 4
BF16 = jnp.bfloat16
F32 = jnp.float32
LOG2E = 1.4426950408889634
MESH = pl.DeviceIdType.MESH

masked_score = -1e30

ROWS_BY_ROWS = (((1,), (1,)), ((), ()))


def dot(a, b):
    return jnp.dot(a, b, preferred_element_type=F32)


def dot_rows(a, b):
    return lax.dot_general(a, b, ROWS_BY_ROWS, preferred_element_type=F32)


def remote(src, dst, send_sem, recv_sem, **where):
    return pltpu.make_async_remote_copy(
        src_ref=src,
        dst_ref=dst,
        send_sem=send_sem,
        recv_sem=recv_sem,
        device_id=where,
        device_id_type=MESH,
    )


def scoped(name):
    def wrap(function):
        @functools.wraps(function)
        def inner(*args):
            with jax.named_scope(name):
                return function(*args)

        return inner

    return wrap


def kernel(sizes, *refs):
    N, L, T, D, KVH, G = (sizes[k] for k in ("N", "L", "T", "D", "KVH", "G"))
    names = sizes["names"]
    r = dict(zip(names, refs))
    C = HD
    NZ = N // 4
    RO = D // (N * L)
    GW = D // N
    R = D // L
    QUARTER, SUB = R // 4, R // 16
    GC = G * C
    scale = HD ** (-0.5)

    n = lax.axis_index("node")
    l = lax.axis_index("local")
    core = lax.rem(n, 2)
    even, odd = core == 0, core == 1
    partner = n + 1 - 2 * core
    xbit = lax.rem(lax.div(n, 2), 2)
    xpeer = n + 2 - 4 * xbit
    z = lax.div(n, 4)
    zbit = lax.rem(z, 2)
    zpeer = n + 4 - 8 * zbit
    has_next, has_prev = n + 2 < N, n >= 2
    has_far_next, has_far_prev = n + 3 < N, n >= 3

    kwin, vwin = r["kwin"], r["vwin"]
    hid, hidp, hid_t, wfull = r["hid"], r["hidp"], r["hid_t"], r["wfull"]

    def rows(offset):
        return pl.ds((DOCB - 1 - offset) * T, T)

    for offset in range(1, DOCB):

        @pl.when(n < offset)
        def _():
            for win in (kwin, vwin):
                for kv in range(KVH):
                    win[kv, rows(offset)] = jnp.zeros((T, C), BF16)

    for name in ("v", "k"):

        @pl.when(n + 2 >= N)
        def _():
            r[name + "_near"][...] = jnp.zeros((KVH, T, C), BF16)

        @pl.when(jnp.logical_and(odd, n + 3 >= N))
        def _():
            r[name + "_third"][...] = jnp.zeros((KVH, T, C), BF16)

    def local_copy(src, dst, sem):
        return pltpu.make_async_copy(src, dst, sem)

    def key_in(kv):
        return local_copy(
            r["keys"].at[:, pl.ds(kv * C, C)], kwin.at[kv, rows(0)], r["key_in_sem"].at[kv]
        )

    def query_in(kv):
        cols = pl.ds(kv * GC, GC)
        return local_copy(r["queries"].at[:, cols], r["q"].at[kv], r["query_in_sem"].at[kv])

    def grad_in(kv):
        cols = pl.ds(kv * GC, GC)
        return local_copy(r["grads"].at[:, cols], r["g"].at[kv], r["grad_in_sem"].at[kv])

    hidden_in = local_copy(r["hidden"], hid, r["in_sem"].at[0])
    weight_in = local_copy(r["weight"], wfull.at[pl.ds(l * R, R)], r["in_sem"].at[1])
    for kv in range(KVH):
        key_in(kv).start()
    hidden_in.start()
    weight_in.start()
    for kv in range(KVH):
        query_in(kv).start()
        grad_in(kv).start()

    barrier = pltpu.get_barrier_semaphore()

    def greet(**where):
        pl.semaphore_signal(barrier, inc=1, device_id=where, device_id_type=MESH)

    greet(node=partner)
    for there, who in (
        (has_next, n + 2),
        (has_prev, n - 2),
        (jnp.logical_and(odd, has_far_next), n + 3),
        (jnp.logical_and(even, has_far_prev), n - 3),
    ):

        @pl.when(there)
        def _():
            greet(node=who)

    for s in range(1, L):
        greet(local=lax.rem(l + s, L))
    for s in range(1, NZ):
        greet(node=lax.rem(n + 4 * s, N))
    as_int = lambda b: jnp.where(b, 1, 0)
    expected = (
        1
        + as_int(has_next)
        + as_int(has_prev)
        + core * as_int(has_far_next)
        + (1 - core) * as_int(has_far_prev)
        + (L - 1)
        + (NZ - 1)
    )
    with jax.named_scope("entry"):
        pl.semaphore_wait(barrier, expected)

    def window(win, name):
        send, recv = r[name + "_send"], r[name + "_recv"]

        def ahead(kv):
            return remote(
                win.at[kv, rows(0)], win.at[kv, rows(2)], send.at[0], recv.at[1, kv], node=n + 2
            )

        def beside(kv):
            return remote(
                win.at[kv, rows(0)], win.at[kv, rows(1)], send.at[1], recv.at[0, kv], node=n + 1
            )

        def far(kv):
            return remote(
                win.at[kv, rows(0)], win.at[kv, rows(3)], send.at[1], recv.at[2, kv], node=n + 3
            )

        def relay_even(kv):
            return remote(
                win.at[kv, rows(2)], win.at[kv, rows(3)], send.at[2], recv.at[2, kv], node=n + 1
            )

        def relay_odd(kv):
            return remote(
                win.at[kv, rows(2)], win.at[kv, rows(1)], send.at[2], recv.at[0, kv], node=n - 1
            )

        far_there = jnp.logical_and(odd, has_far_next)
        relay_e = jnp.logical_and(even, has_prev)
        relay_o = jnp.logical_and(odd, has_prev)

        @scoped(name + "_start")
        def start(kv):
            pl.when(has_next)(lambda: ahead(kv).start())
            pl.when(far_there)(lambda: far(kv).start())
            pl.when(even)(lambda: beside(kv).start())

        @scoped(name + "_relay")
        def relay(kv):
            @pl.when(has_prev)
            def _():
                ahead(kv).wait_recv()

            pl.when(relay_e)(lambda: relay_even(kv).start())
            pl.when(relay_o)(lambda: relay_odd(kv).start())

        @scoped(name + "_wait")
        def wait(kv):
            pl.when(jnp.logical_or(odd, has_prev))(lambda: beside(kv).wait_recv())
            pl.when(has_far_prev)(lambda: far(kv).wait_recv())

        def drain():
            def sent(kind, place):
                part = win.at[:, rows(place)]
                return remote(part, part, send.at[kind], recv.at[0, 0], node=partner)

            pl.when(has_next)(lambda: sent(0, 0).wait_send())
            pl.when(jnp.logical_or(even, has_far_next))(lambda: sent(1, 0).wait_send())
            pl.when(has_prev)(lambda: sent(2, 2).wait_send())

        return start, relay, wait, drain

    key_start, key_relay, key_wait, key_drain = window(kwin, "kw")
    value_start, value_relay, value_wait, value_drain = window(vwin, "vw")

    for kv in range(2):
        key_in(kv).wait()
        key_start(kv)

    def weight_part(owner, zb, xb, sub):
        return pl.ds(owner * R + (zb * 2 + xb) * QUARTER + (core * 2 + sub) * SUB, SUB)

    def weight_class(owner, index):
        if index < 2:
            return weight_part(owner, zbit, xbit, index)
        return weight_part(owner, 1 - zbit, 1 - xbit, index - 2)

    def weight_start(s, index):
        return remote(
            r["weight"].at[weight_class(0, index)],
            wfull.at[weight_class(l, index)],
            r["w_send"].at[0, s - 1],
            r["w_recv"].at[0, L - s - 1, index],
            local=lax.rem(l + s, L),
        )

    def weight_pass(s, index, kind):
        owner = lax.rem(l + s, L)
        if kind <= 3:
            rows_at = weight_class(owner, index)
        elif kind == 4:
            rows_at = weight_part(owner, 1 - zbit, xbit, index)
        else:
            rows_at = weight_part(owner, zbit, 1 - xbit, index)
        part = wfull.at[rows_at]
        return remote(
            part,
            part,
            r["w_send"].at[kind, s - 1],
            r["w_recv"].at[kind, s - 1, index],
            node={1: zpeer, 2: xpeer}.get(kind, partner),
        )

    @scoped("weight_relay")
    def weight_relay(index):
        for s in range(1, L):
            weight_start(L - s, index).wait_recv()
            if index < 2:
                weight_pass(s, index, 1).start()
                weight_pass(s, index, 2).start()
            weight_pass(s, index, 3).start()

    @scoped("weight_again")
    def weight_relay_again(sub):
        for s in range(1, L):
            weight_pass(s, sub, 1).wait_recv()
            weight_pass(s, sub, 4).start()
            weight_pass(s, sub, 2).wait_recv()
            weight_pass(s, sub, 5).start()

    weight_kinds = [(k, i) for k in (3, 1, 2, 4, 5) for i in range(4) if k == 3 or i < 2]

    for sub in range(4):
        for s in range(1, L):
            weight_start(s, sub).start()

    def hidden_swap(j):
        cols = pl.ds((2 * j + 1 - core) * GW, GW)
        return remote(
            r["hidden"].at[:, cols], hidp.at[j], r["h_send"], r["h_recv"], node=partner
        )

    def hidden_all():
        return remote(hidp, hidp, r["h_send"], r["h_recv"], node=partner)

    block = n

    def find(j, carry):
        first, start, length = carry
        size = r["lengths"][0, r["order"][0, j]]
        count = lax.div(size + (T - 1), T)
        inside = jnp.logical_and(first <= block, block < first + count)
        return (
            first + count,
            jnp.where(inside, first, start),
            jnp.where(inside, size, length),
        )

    zero = jnp.int32(0)
    _, doc_start, doc_length = lax.fori_loop(0, r["lengths"].shape[1], find, (zero, zero, zero))
    low = (doc_start - block + (DOCB - 1)) * T
    high = low + doc_length
    key_at = lax.broadcasted_iota(jnp.int32, (DOCB * T, T), 0)
    query_at = lax.broadcasted_iota(jnp.int32, (DOCB * T, T), 1) + (DOCB - 1) * T
    allowed = (key_at >= low) & (key_at < high) & (key_at <= query_at)
    r["bias"][...] = jnp.where(allowed, 0.0, masked_score)
    query_row = lax.broadcasted_iota(jnp.int32, (T, GC), 0) + (DOCB - 1) * T
    query_ok = query_row < high

    with jax.named_scope("hid_in"):
        hidden_in.wait()
    weight_in.wait()
    with jax.named_scope("turn_hid"):
      for j in range(N // 2):
        cols = pl.ds(pl.multiple_of((2 * j + core) * GW, GW), GW)
        hid_t[pl.ds(j * GW, GW), 0:T] = hid[:, cols].T
    own_cols = pl.ds(pl.multiple_of(l * R, R), R)
    with jax.named_scope("half_values"):
        r["vacc"][...] = dot(hid[:, own_cols], wfull[pl.ds(pl.multiple_of(l * R, R), R)])
    for kv in range(KVH):
        query_in(kv).wait()
        grad_in(kv).wait()
    with jax.named_scope("mask_g"):
      for kv in range(KVH):
        r["g"][kv] = jnp.where(query_ok, r["g"][kv].astype(F32), 0.0).astype(BF16)

    def backward(name):
        send, recv = r[name + "_send"], r[name + "_recv"]
        out, mid, comb = r[name + "_out"], r[name + "_mid"], r[name + "_comb"]
        near, third, own, keep = (r[name + e] for e in ("_near", "_third", "_own", "_keep"))
        to_third = jnp.logical_or(odd, has_far_prev)
        third_node = jnp.where(even, n - 3, n - 1)
        from_third = jnp.logical_or(even, has_far_next)

        def across(kv):
            return remote(out.at[kv, 0], mid.at[kv], send.at[0], recv.at[0, kv], node=partner)

        def skip(kv):
            return remote(
                out.at[kv, 1], third.at[kv], send.at[1], recv.at[1, kv], node=third_node
            )

        def back(kv):
            return remote(comb.at[kv], near.at[kv], send.at[2], recv.at[2, kv], node=n - 2)

        @scoped(name + "_give")
        def give(kv, acc):
            out[kv, 0] = acc[pl.ds((1 - core) * 2 * T, T)].astype(BF16)
            out[kv, 1] = acc[pl.ds(core * 2 * T, T)].astype(BF16)
            across(kv).start()
            pl.when(to_third)(lambda: skip(kv).start())
            keep[kv] = acc[rows(2)]
            own[kv] = acc[rows(0)]

        @scoped(name + "_combine")
        def combine(kv):
            across(kv).wait_recv()

            @pl.when(has_prev)
            def _():
                comb[kv] = (keep[kv] + mid[kv].astype(F32)).astype(BF16)
                back(kv).start()

        def total(kv):
            pl.when(from_third)(lambda: skip(kv).wait_recv())
            pl.when(has_next)(lambda: back(kv).wait_recv())
            return own[kv] + near[kv].astype(F32) + third[kv].astype(F32)

        def drain():
            def sent(kind, part):
                return remote(part, part, send.at[kind], recv.at[0, 0], node=partner)

            sent(0, out.at[:, 0]).wait_send()
            pl.when(to_third)(lambda: sent(1, out.at[:, 1]).wait_send())
            pl.when(has_prev)(lambda: sent(2, comb).wait_send())

        return give, combine, total, drain

    v_give, v_combine, v_total, v_drain = backward("v")
    k_give, k_combine, k_total, k_drain = backward("k")

    vl = r["vl"]

    def low_swap(kv):
        return remote(
            vl.at[kv, pl.ds(0, T)],
            vl.at[kv, pl.ds(T, T)],
            r["vl_send"],
            r["vl_recv"].at[kv],
            node=partner,
        )

    @scoped("value_own")
    def value_own(kv):
        vl[kv, 0:T] = v_total(kv).astype(BF16)
        low_swap(kv).start()

    wacc, xk = r["wacc"], r["xk"]
    ys, yr, xs, xr, zs, zr = (r[k] for k in ("ys", "yr", "xs", "xr", "zs", "zr"))

    def y_copy(kv, h, s):
        return remote(
            ys.at[s - 1, kv, h],
            yr.at[L - s - 1, kv, h],
            r["y_send"].at[s - 1],
            r["y_recv"].at[L - s - 1, kv, h],
            local=lax.rem(l + s, L),
        )

    def x_copy(kv, h):
        return remote(xs.at[kv, h], xr.at[kv, h], r["x_send"], r["x_recv"].at[kv, h], node=xpeer)

    def z_copy(kv, s, h):
        there = lax.rem(z + s, NZ)
        return remote(
            zs.at[kv, h, lax.div(there, 2)],
            zr.at[NZ - s - 1, kv],
            r["z_send"].at[s - 1],
            r["z_recv"].at[NZ - s - 1, kv],
            node=lax.rem(n + 4 * s, N),
        )

    @scoped("terms")
    def grad_terms(kv):
        low_swap(kv).wait_recv()
        both = vl[kv]
        for h in range(2):
            for i in range(NZ // 2):
                for x in range(2):
                    j = (2 * i + h) * 2 + x
                    part = dot(hid_t[pl.ds(j * GW, GW)], both)
                    wacc[kv, j] = part.reshape(L, RO, C)
                    for s in range(1, L):
                        ys[s - 1, kv, h, i, x] = wacc[kv, j, lax.rem(l + s, L)].astype(BF16)
            for s in range(1, L):
                y_copy(kv, h, s).start()

    @scoped("second")
    def grad_second(kv, h):
        for s in range(1, L):
            y_copy(kv, h, L - s).wait_recv()

        def summed(i, x):
            total = wacc[kv, (2 * i + h) * 2 + x, l]
            for s in range(1, L):
                total = total + yr[s - 1, kv, h, i, x].astype(F32)
            return total

        for i in range(NZ // 2):
            xs[kv, h, i] = summed(i, 1 - xbit).astype(BF16)
        x_copy(kv, h).start()
        for i in range(NZ // 2):
            xk[kv, h, i] = summed(i, xbit)

    @scoped("third")
    def grad_third(kv, h):
        x_copy(kv, h).wait_recv()
        for i in range(NZ // 2):
            total = xk[kv, h, i] + xr[kv, h, i].astype(F32)
            xk[kv, h, i] = total
            zs[kv, h, i] = total.astype(BF16)
        for s in range(1, NZ):

            @pl.when(lax.rem(z + s, 2) == h)
            def _():
                z_copy(kv, s, h).start()

    @scoped("final")
    def grad_final(kv):
        for s in range(1, NZ):
            z_copy(kv, NZ - s, 0).wait_recv()
        total = xk[kv, zbit, lax.div(z, 2)]
        for s in range(1, NZ):
            total = total + zr[s - 1, kv].astype(F32)
        r["weight_grad"][kv] = total

    @scoped("key_own")
    def key_own(kv):
        r["key_grad"][kv] = k_total(kv).astype(BF16)

    probs, acc = r["probs"], r["acc"]

    @scoped("value_heads")
    def value_heads(kv, heads):
        keys = kwin[kv]
        for head in heads:
            cols = slice(head * C, (head + 1) * C)
            scores = dot_rows(keys, r["q"][kv, :, cols]) + r["bias"][...]
            top = jnp.max(scores, axis=0, keepdims=True)
            expd = jnp.exp2((scores - top) * (scale * LOG2E))
            low_probs = (expd * (1.0 / jnp.sum(expd, axis=0, keepdims=True))).astype(BF16)
            probs[kv * G + head] = low_probs
            part = dot(low_probs, r["g"][kv, :, cols])
            if head == 0:
                acc[...] = part
            else:
                acc[...] += part

    @scoped("key_heads")
    def key_heads(kv, heads):
        values = vwin[kv]
        turned = kwin[kv].T
        for head in heads:
            cols = slice(head * C, (head + 1) * C)
            prob_grad = dot_rows(values, r["g"][kv, :, cols])
            p = probs[kv * G + head].astype(F32)
            delta = jnp.sum(p * prob_grad, axis=0, keepdims=True)
            score_grad = (p * (prob_grad - delta) * scale).astype(BF16)
            r["query_grad"][kv, :, cols] = dot(turned, score_grad).T.astype(BF16)
            part = dot(score_grad, r["q"][kv, :, cols])
            if head == 0:
                acc[...] = part
            else:
                acc[...] += part

    half = G // 2
    first_heads, last_heads = tuple(range(half)), tuple(range(half, G))
    last = KVH - 1

    def at(kv, plan):
        for when_kv in sorted({k for k, *_ in plan}):

            @pl.when(kv == when_kv)
            def _():
                for k, task, *args in plan:
                    if k == when_kv:
                        task(*args)

    @scoped("partner_hid")
    def partner_hidden():
        hidden_all().wait_recv()
        for j in range(N // 2):
            hid_t[pl.ds(j * GW, GW), T : 2 * T] = hidp[j].T

    def more_keys(kv):
        key_in(kv).wait()
        key_start(kv)

    key_relay(0)
    for j in range(N // 2):
        hidden_swap(j).start()

    value_start_plan = [(kv, more_keys, kv + 2) for kv in range(KVH - 2)]
    value_mid_plan = (
        [(kv, key_relay, kv + 1) for kv in range(KVH - 1)]
        + [(kv, v_combine, kv - 1) for kv in range(1, KVH)]
        + [(kv, weight_relay, kv) for kv in range(KVH)]
        + [(1, partner_hidden)]
        + [(2, weight_relay_again, 0)]
        + [(kv, value_own, kv - 2) for kv in range(2, KVH)]
    )
    value_end_plan = [(kv, grad_terms, kv - 2) for kv in range(2, KVH)]

    def value_pass(kv, carry):
        key_wait(kv)
        at(kv, value_start_plan)
        value_heads(kv, first_heads)
        at(kv, value_mid_plan)
        value_heads(kv, last_heads)
        v_give(kv, acc)
        at(kv, value_end_plan)
        return carry

    lax.fori_loop(0, KVH, value_pass, 0)

    weight_relay_again(1)
    v_combine(last)
    value_own(2)

    with jax.named_scope("weight_wait"):
        for s in range(1, L):
            for kind, index in weight_kinds:
                if kind >= 3:
                    weight_pass(s, index, kind).wait_recv()
    with jax.named_scope("rest_values"):
        values = r["vacc"][...]
        for s in range(1, L):
            there = pl.multiple_of(lax.rem(l + s, L) * R, R)
            values = values + dot(hid[:, pl.ds(there, R)], wfull[pl.ds(there, R)])
        for kv in range(KVH):
            vwin[kv, rows(0)] = values[:, kv * C : (kv + 1) * C].astype(BF16)
    for kv in range(KVH):
        value_start(kv)
    grad_terms(2)
    grad_second(0, 0)
    value_own(last)

    step = D // 8

    def input_passes(low, high):
        own_low = jnp.concatenate([vl[kv, 0:T] for kv in range(KVH)], axis=1)

        def input_pass(i, carry):
            at = pl.multiple_of(i * step, step)
            r["input_grad"][:, pl.ds(at, step)] = dot_rows(own_low, wfull[pl.ds(at, step)]).astype(BF16)
            return carry

        with jax.named_scope("input_grad"):
            lax.fori_loop(low, high, input_pass, 0)

    input_passes(0, 4)
    value_relay(0)
    grad_terms(last)
    grad_second(0, 1)

    key_mid_plan = (
        [(kv, value_relay, kv + 1) for kv in range(KVH - 1)]
        + [(kv, k_combine, kv - 1) for kv in range(1, KVH)]
        + [
            (0, grad_second, 1, 0),
            (2, grad_second, 3, 0),
            (1, grad_third, 0, 0),
            (1, grad_third, 0, 1),
            (2, grad_third, 1, 1),
            (2, grad_third, 2, 0),
            (3, grad_third, 3, 0),
        ]
    )
    key_end_plan = [
        (0, grad_second, 1, 1),
        (0, grad_second, 2, 0),
        (1, grad_second, 2, 1),
        (1, grad_third, 1, 0),
        (2, grad_second, 3, 1),
        (2, grad_third, 2, 1),
        (3, grad_third, 3, 1),
        (3, grad_final, 0),
    ] + [(kv, key_own, kv - 2) for kv in range(2, KVH)]

    def key_pass(kv, carry):
        value_wait(kv)
        key_heads(kv, first_heads)
        at(kv, key_mid_plan)
        key_heads(kv, last_heads)
        k_give(kv, acc)
        at(kv, key_end_plan)
        return carry

    lax.fori_loop(0, KVH, key_pass, 0)
    input_passes(4, 8)
    k_combine(last)
    grad_final(1)
    grad_final(2)
    key_own(last - 1)
    key_own(last)
    grad_final(last)

    for drain in (key_drain, value_drain, v_drain, k_drain):
        drain()
    remote(vl.at[:, 0:T], vl.at[:, 0:T], r["vl_send"], r["vl_recv"].at[0], node=partner).wait_send()
    for s in range(1, L):
        remote(
            ys.at[s - 1], ys.at[s - 1], r["y_send"].at[s - 1], r["y_recv"].at[0, 0, 0], node=partner
        ).wait_send()
        for kind in range(6):
            part = wfull.at[pl.ds(0, SUB * (4 if kind in (0, 3) else 2))]
            remote(
                part, part, r["w_send"].at[kind, s - 1], r["w_recv"].at[0, 0, 0], node=partner
            ).wait_send()
    remote(xs, xs, r["x_send"], r["x_recv"].at[0, 0], node=partner).wait_send()
    for s in range(1, NZ):
        part = zs.at[:, 0, 0]
        remote(
            part, part, r["z_send"].at[s - 1], r["z_recv"].at[0, 0], node=partner
        ).wait_send()
    hidden_all().wait_send()


def local(hidden, queries, saved_keys, grad_out, value_weight, doc_lengths, doc_order):
    N, L = lax.axis_size("node"), lax.axis_size("local")
    T, D = hidden.shape[1:]
    QW, KVW = queries.shape[2], saved_keys.shape[2]
    KVH = KVW // HD
    G = QW // KVW
    C = HD
    NZ, RO, GW, J = N // 4, D // (N * L), D // N, N // 2
    vmem = lambda *shape: lambda dtype: pltpu.VMEM(shape, dtype)
    dma = lambda *shape: pltpu.SemaphoreType.DMA(shape)
    scratch = dict(
        kwin=pltpu.VMEM((KVH, DOCB * T, C), BF16),
        vwin=pltpu.VMEM((KVH, DOCB * T, C), BF16),
        q=pltpu.VMEM((KVH, T, G * C), BF16),
        g=pltpu.VMEM((KVH, T, G * C), BF16),
        hid=pltpu.VMEM((T, D), BF16),
        hidp=pltpu.VMEM((J, T, GW), BF16),
        hid_t=pltpu.VMEM((J * GW, 2 * T), BF16),
        wfull=pltpu.VMEM((D, KVW), BF16),
        bias=pltpu.VMEM((DOCB * T, T), F32),
        vacc=pltpu.VMEM((T, KVW), F32),
        probs=pltpu.VMEM((KVH * G, DOCB * T, T), BF16),
        acc=pltpu.VMEM((DOCB * T, C), F32),
        vl=pltpu.VMEM((KVH, 2 * T, C), BF16),
        wacc=pltpu.VMEM((KVH, J, L, RO, C), F32),
        ys=pltpu.VMEM((L - 1, KVH, 2, NZ // 2, 2, RO, C), BF16),
        yr=pltpu.VMEM((L - 1, KVH, 2, NZ // 2, 2, RO, C), BF16),
        xs=pltpu.VMEM((KVH, 2, NZ // 2, RO, C), BF16),
        xr=pltpu.VMEM((KVH, 2, NZ // 2, RO, C), BF16),
        xk=pltpu.VMEM((KVH, 2, NZ // 2, RO, C), F32),
        zs=pltpu.VMEM((KVH, 2, NZ // 2, RO, C), BF16),
        zr=pltpu.VMEM((NZ - 1, KVH, RO, C), BF16),
        key_in_sem=dma(KVH),
        query_in_sem=dma(KVH),
        grad_in_sem=dma(KVH),
        in_sem=dma(2),
        w_send=dma(6, L - 1),
        w_recv=dma(6, L - 1, 4),
        h_send=pltpu.SemaphoreType.DMA,
        h_recv=pltpu.SemaphoreType.DMA,
        vl_send=pltpu.SemaphoreType.DMA,
        vl_recv=dma(KVH),
        y_send=dma(L - 1),
        y_recv=dma(L - 1, KVH, 2),
        x_send=pltpu.SemaphoreType.DMA,
        x_recv=dma(KVH, 2),
        z_send=dma(NZ - 1),
        z_recv=dma(NZ - 1, KVH),
    )
    for name in ("kw", "vw", "v", "k"):
        scratch[name + "_send"] = dma(3)
        scratch[name + "_recv"] = dma(3, KVH)
    for name in ("v", "k"):
        scratch[name + "_out"] = pltpu.VMEM((KVH, 2, T, C), BF16)
        for extra in ("_mid", "_comb", "_near", "_third"):
            scratch[name + extra] = pltpu.VMEM((KVH, T, C), BF16)
        for extra in ("_own", "_keep"):
            scratch[name + extra] = pltpu.VMEM((KVH, T, C), F32)
    args = ("lengths", "order", "hidden", "queries", "keys", "grads", "weight")
    outs = ("query_grad", "key_grad", "input_grad", "weight_grad")
    sizes = dict(N=N, L=L, T=T, D=D, KVH=KVH, G=G, names=args + outs + tuple(scratch))
    smem = pl.BlockSpec(memory_space=pltpu.SMEM)
    anywhere = pl.BlockSpec(memory_space=pltpu.HBM)
    held = pl.BlockSpec(memory_space=pltpu.VMEM)
    grads = pl.pallas_call(
        functools.partial(kernel, sizes),
        out_shape=[
            pltpu.VMEM((KVH, T, G * C), BF16),
            pltpu.VMEM((KVH, T, C), BF16),
            pltpu.VMEM((T, D), BF16),
            pltpu.VMEM((KVH, RO, C), F32),
        ],
        in_specs=[smem, smem] + [anywhere] * 5,
        out_specs=[held] * 4,
        scratch_shapes=list(scratch.values()),
        compiler_params=pltpu.CompilerParams(
            collective_id=0, has_side_effects=True, vmem_limit_bytes=60 * 2**20
        ),
        name="attention_grads",
    )(
        doc_lengths,
        doc_order,
        hidden[0],
        queries[0],
        saved_keys[0],
        grad_out[0],
        value_weight,
    )
    return results(
        grads,
        [
            jax.ShapeDtypeStruct((1, T, QW), BF16),
            jax.ShapeDtypeStruct((1, T, KVW), BF16),
            jax.ShapeDtypeStruct((1, T, D), BF16),
            jax.ShapeDtypeStruct((RO, KVW), F32),
        ],
    )


def results_kernel(query_in, key_in, input_in, weight_in, query, key, x, weight, sems):
    copies = [(input_in, x.at[0])]
    for kv in range(query_in.shape[0]):
        for a, b in ((query_in, query.at[0]), (key_in, key.at[0]), (weight_in, weight)):
            width = a.shape[2]
            copies.append((a.at[kv], b.at[:, pl.ds(kv * width, width)]))
    copies = [pltpu.make_async_copy(a, b, sems.at[i]) for i, (a, b) in enumerate(copies)]
    for copy in copies:
        copy.start()
    for copy in copies:
        copy.wait()


def results(arrays, shapes):
    heads = arrays[0].shape[0]
    return pl.pallas_call(
        results_kernel,
        out_shape=shapes,
        in_specs=[pl.BlockSpec(memory_space=pltpu.VMEM)] * len(arrays),
        out_specs=[pl.BlockSpec(memory_space=pl.ANY)] * len(arrays),
        scratch_shapes=[pltpu.SemaphoreType.DMA((1 + 3 * heads,))],
        compiler_params=pltpu.CompilerParams(vmem_limit_bytes=2**20),
        name="results",
    )(*arrays)


def solution(mesh):
    tokens = P("local", "node", None)
    return jax.shard_map(
        local,
        mesh=mesh,
        in_specs=(tokens,) * 4 + (P("local", None),) * 3,
        out_specs=(tokens,) * 3 + (P(("node", "local"), None),),
        check_vma=False,
    )
```

```python
import functools

import jax
import jax.numpy as jnp
from jax import lax
from jax.experimental import pallas as pl
from jax.experimental.pallas import tpu as pltpu
from jax.sharding import PartitionSpec as P

HD = 128
DOCB = 4
BF16 = jnp.bfloat16
F32 = jnp.float32
LOG2E = 1.4426950408889634
MESH = pl.DeviceIdType.MESH

masked_score = -1e30

ROWS_BY_ROWS = (((1,), (1,)), ((), ()))


def dot(a, b):
    return jnp.dot(a, b, preferred_element_type=F32)


def dot_rows(a, b):
    return lax.dot_general(a, b, ROWS_BY_ROWS, preferred_element_type=F32)


def remote(src, dst, send_sem, recv_sem, **where):
    return pltpu.make_async_remote_copy(
        src_ref=src,
        dst_ref=dst,
        send_sem=send_sem,
        recv_sem=recv_sem,
        device_id=where,
        device_id_type=MESH,
    )


def scoped(name):
    def wrap(function):
        @functools.wraps(function)
        def inner(*args):
            with jax.named_scope(name):
                return function(*args)

        return inner

    return wrap


def kernel(sizes, *refs):
    N, L, T, D, KVH, G = (sizes[k] for k in ("N", "L", "T", "D", "KVH", "G"))
    names = sizes["names"]
    r = dict(zip(names, refs))
    C = HD
    NZ = N // 4
    RO = D // (N * L)
    GW = D // N
    R = D // L
    QUARTER, SUB = R // 4, R // 16
    GC = G * C
    scale = HD ** (-0.5)

    n = lax.axis_index("node")
    l = lax.axis_index("local")
    core = lax.rem(n, 2)
    even, odd = core == 0, core == 1
    partner = n + 1 - 2 * core
    xbit = lax.rem(lax.div(n, 2), 2)
    xpeer = n + 2 - 4 * xbit
    z = lax.div(n, 4)
    zbit = lax.rem(z, 2)
    zpeer = n + 4 - 8 * zbit
    has_next, has_prev = n + 2 < N, n >= 2
    has_far_next, has_far_prev = n + 3 < N, n >= 3

    kwin, vwin = r["kwin"], r["vwin"]
    hid, hidp, hid_t, wfull = r["hid"], r["hidp"], r["hid_t"], r["wfull"]

    def rows(offset):
        return pl.ds((DOCB - 1 - offset) * T, T)

    for offset in range(1, DOCB):

        @pl.when(n < offset)
        def _():
            for win in (kwin, vwin):
                for kv in range(KVH):
                    win[kv, rows(offset)] = jnp.zeros((T, C), BF16)

    for name in ("v", "k"):

        @pl.when(n + 2 >= N)
        def _():
            r[name + "_near"][...] = jnp.zeros((KVH, T, C), BF16)

        @pl.when(jnp.logical_and(odd, n + 3 >= N))
        def _():
            r[name + "_third"][...] = jnp.zeros((KVH, T, C), BF16)

    def local_copy(src, dst, sem):
        return pltpu.make_async_copy(src, dst, sem)

    def key_in(kv):
        return local_copy(
            r["keys"].at[:, pl.ds(kv * C, C)], kwin.at[kv, rows(0)], r["key_in_sem"].at[kv]
        )

    def head_copies(source, into, sem, kv):
        return [
            local_copy(
                r[source].at[:, pl.ds(kv * GC + head * C, C)],
                r[into].at[kv, pl.ds(head * T, T)],
                r[sem].at[kv],
            )
            for head in range(G)
        ]

    def heads_wait(into, sem, kv):
        local_copy(r[into].at[kv], r[into].at[kv], r[sem].at[kv]).wait()

    hidden_in = local_copy(r["hidden"], hid, r["in_sem"].at[0])
    weight_in = local_copy(r["weight"], wfull.at[pl.ds(l * R, R)], r["in_sem"].at[1])
    for kv in range(KVH):
        key_in(kv).start()
    hidden_in.start()
    weight_in.start()
    for kv in range(KVH):
        for copy in head_copies("queries", "q", "query_in_sem", kv):
            copy.start()
        for copy in head_copies("grads", "g", "grad_in_sem", kv):
            copy.start()

    barrier = pltpu.get_barrier_semaphore()

    def greet(**where):
        pl.semaphore_signal(barrier, inc=1, device_id=where, device_id_type=MESH)

    greet(node=partner)
    for there, who in (
        (has_next, n + 2),
        (has_prev, n - 2),
        (jnp.logical_and(odd, has_far_next), n + 3),
        (jnp.logical_and(even, has_far_prev), n - 3),
    ):

        @pl.when(there)
        def _():
            greet(node=who)

    for s in range(1, L):
        greet(local=lax.rem(l + s, L))
    for s in range(1, NZ):
        greet(node=lax.rem(n + 4 * s, N))
    as_int = lambda b: jnp.where(b, 1, 0)
    expected = (
        1
        + as_int(has_next)
        + as_int(has_prev)
        + core * as_int(has_far_next)
        + (1 - core) * as_int(has_far_prev)
        + (L - 1)
        + (NZ - 1)
    )
    with jax.named_scope("entry"):
        pl.semaphore_wait(barrier, expected)

    def window(win, name):
        send, recv = r[name + "_send"], r[name + "_recv"]

        def ahead(kv):
            return remote(
                win.at[kv, rows(0)], win.at[kv, rows(2)], send.at[0], recv.at[1, kv], node=n + 2
            )

        def beside(kv):
            return remote(
                win.at[kv, rows(0)], win.at[kv, rows(1)], send.at[1], recv.at[0, kv], node=n + 1
            )

        def far(kv):
            return remote(
                win.at[kv, rows(0)], win.at[kv, rows(3)], send.at[1], recv.at[2, kv], node=n + 3
            )

        def relay_even(kv):
            return remote(
                win.at[kv, rows(2)], win.at[kv, rows(3)], send.at[2], recv.at[2, kv], node=n + 1
            )

        def relay_odd(kv):
            return remote(
                win.at[kv, rows(2)], win.at[kv, rows(1)], send.at[2], recv.at[0, kv], node=n - 1
            )

        far_there = jnp.logical_and(odd, has_far_next)
        relay_e = jnp.logical_and(even, has_prev)
        relay_o = jnp.logical_and(odd, has_prev)

        @scoped(name + "_start")
        def start(kv):
            pl.when(has_next)(lambda: ahead(kv).start())
            pl.when(far_there)(lambda: far(kv).start())
            pl.when(even)(lambda: beside(kv).start())

        @scoped(name + "_relay")
        def relay(kv):
            @pl.when(has_prev)
            def _():
                ahead(kv).wait_recv()

            pl.when(relay_e)(lambda: relay_even(kv).start())
            pl.when(relay_o)(lambda: relay_odd(kv).start())

        @scoped(name + "_wait")
        def wait(kv):
            pl.when(jnp.logical_or(odd, has_prev))(lambda: beside(kv).wait_recv())
            pl.when(has_far_prev)(lambda: far(kv).wait_recv())

        def drain():
            def sent(kind, place):
                part = win.at[:, rows(place)]
                return remote(part, part, send.at[kind], recv.at[0, 0], node=partner)

            pl.when(has_next)(lambda: sent(0, 0).wait_send())
            pl.when(jnp.logical_or(even, has_far_next))(lambda: sent(1, 0).wait_send())
            pl.when(has_prev)(lambda: sent(2, 2).wait_send())

        return start, relay, wait, drain

    key_start, key_relay, key_wait, key_drain = window(kwin, "kw")
    value_start, value_relay, value_wait, value_drain = window(vwin, "vw")

    for kv in range(KVH):
        key_in(kv).wait()
        key_start(kv)

    def weight_part(owner, zb, xb, sub):
        return pl.ds(owner * R + (zb * 2 + xb) * QUARTER + (core * 2 + sub) * SUB, SUB)

    def weight_class(owner, index):
        if index < 2:
            return weight_part(owner, zbit, xbit, index)
        return weight_part(owner, 1 - zbit, 1 - xbit, index - 2)

    def weight_start(s, index):
        return remote(
            r["weight"].at[weight_class(0, index)],
            wfull.at[weight_class(l, index)],
            r["w_send"].at[0, s - 1],
            r["w_recv"].at[0, L - s - 1, index],
            local=lax.rem(l + s, L),
        )

    def weight_pass(s, index, kind):
        owner = lax.rem(l + s, L)
        if kind <= 3:
            rows_at = weight_class(owner, index)
        elif kind == 4:
            rows_at = weight_part(owner, 1 - zbit, xbit, index)
        else:
            rows_at = weight_part(owner, zbit, 1 - xbit, index)
        part = wfull.at[rows_at]
        return remote(
            part,
            part,
            r["w_send"].at[kind, s - 1],
            r["w_recv"].at[kind, s - 1, index],
            node={1: zpeer, 2: xpeer}.get(kind, partner),
        )

    @scoped("weight_relay")
    def weight_relay(index):
        for s in range(1, L):
            weight_start(L - s, index).wait_recv()
            if index < 2:
                weight_pass(s, index, 1).start()
                weight_pass(s, index, 2).start()
            weight_pass(s, index, 3).start()

    @scoped("weight_again")
    def weight_relay_again(sub):
        for s in range(1, L):
            weight_pass(s, sub, 1).wait_recv()
            weight_pass(s, sub, 4).start()
            weight_pass(s, sub, 2).wait_recv()
            weight_pass(s, sub, 5).start()

    weight_kinds = [(k, i) for k in (3, 1, 2, 4, 5) for i in range(4) if k == 3 or i < 2]

    for sub in range(4):
        for s in range(1, L):
            weight_start(s, sub).start()

    def hidden_swap(j):
        cols = pl.ds((2 * j + 1 - core) * GW, GW)
        return remote(
            r["hidden"].at[:, cols], hidp.at[j], r["h_send"], r["h_recv"], node=partner
        )

    def hidden_all():
        return remote(hidp, hidp, r["h_send"], r["h_recv"], node=partner)

    block = n

    def find(j, carry):
        first, start, length = carry
        size = r["lengths"][0, r["order"][0, j]]
        count = lax.div(size + (T - 1), T)
        inside = jnp.logical_and(first <= block, block < first + count)
        return (
            first + count,
            jnp.where(inside, first, start),
            jnp.where(inside, size, length),
        )

    zero = jnp.int32(0)
    _, doc_start, doc_length = lax.fori_loop(0, r["lengths"].shape[1], find, (zero, zero, zero))
    low = (doc_start - block + (DOCB - 1)) * T
    high = low + doc_length
    key_at = lax.broadcasted_iota(jnp.int32, (DOCB * T, C), 0)
    outside = jnp.logical_or(key_at < low, key_at >= high)
    r["outside"][...] = jnp.where(outside, masked_score, 0.0)
    later = lax.broadcasted_iota(jnp.int32, (T, T), 0) > lax.broadcasted_iota(jnp.int32, (T, T), 1)
    r["bias"][...] = jnp.where(later, masked_score, 0.0)
    query_row = lax.broadcasted_iota(jnp.int32, (T, C), 0) + (DOCB - 1) * T
    query_ok = query_row < high

    with jax.named_scope("hid_in"):
        hidden_in.wait()
    weight_in.wait()
    with jax.named_scope("turn_hid"):
      for j in range(N // 2):
        cols = pl.ds(pl.multiple_of((2 * j + core) * GW, GW), GW)
        hid_t[pl.ds(j * GW, GW), 0:T] = hid[:, cols].T
    own_cols = pl.ds(pl.multiple_of(l * R, R), R)
    with jax.named_scope("half_values"):
        r["vacc"][...] = dot(hid[:, own_cols], wfull[pl.ds(pl.multiple_of(l * R, R), R)])
    for kv in range(KVH):
        heads_wait("q", "query_in_sem", kv)
        heads_wait("g", "grad_in_sem", kv)
    with jax.named_scope("mask_g"):
      for kv in range(KVH):
        for head in range(G):
            at_rows = pl.ds(head * T, T)
            masked = jnp.where(query_ok, r["g"][kv, at_rows].astype(F32), 0.0)
            r["g"][kv, at_rows] = masked.astype(BF16)

    def backward(name, factor):
        send, recv = r[name + "_send"], r[name + "_recv"]
        out, mid, comb = r[name + "_out"], r[name + "_mid"], r[name + "_comb"]
        near, third, own, keep = (r[name + e] for e in ("_near", "_third", "_own", "_keep"))
        to_third = jnp.logical_or(odd, has_far_prev)
        third_node = jnp.where(even, n - 3, n - 1)
        from_third = jnp.logical_or(even, has_far_next)

        def across(kv):
            return remote(out.at[kv, 0], mid.at[kv], send.at[0], recv.at[0, kv], node=partner)

        def skip(kv):
            return remote(
                out.at[kv, 1], third.at[kv], send.at[1], recv.at[1, kv], node=third_node
            )

        def back(kv):
            return remote(comb.at[kv], near.at[kv], send.at[2], recv.at[2, kv], node=n - 2)

        @scoped(name + "_give")
        def give(kv, acc):
            out[kv, 0] = (acc[pl.ds((1 - core) * 2 * T, T)] * factor).astype(BF16)
            out[kv, 1] = (acc[pl.ds(core * 2 * T, T)] * factor).astype(BF16)
            across(kv).start()
            pl.when(to_third)(lambda: skip(kv).start())
            keep[kv] = acc[rows(2)] * factor
            own[kv] = acc[rows(0)] * factor

        @scoped(name + "_combine")
        def combine(kv):
            across(kv).wait_recv()

            @pl.when(has_prev)
            def _():
                comb[kv] = (keep[kv] + mid[kv].astype(F32)).astype(BF16)
                back(kv).start()

        def total(kv):
            pl.when(from_third)(lambda: skip(kv).wait_recv())
            pl.when(has_next)(lambda: back(kv).wait_recv())
            return own[kv] + near[kv].astype(F32) + third[kv].astype(F32)

        def drain():
            def sent(kind, part):
                return remote(part, part, send.at[kind], recv.at[0, 0], node=partner)

            sent(0, out.at[:, 0]).wait_send()
            pl.when(to_third)(lambda: sent(1, out.at[:, 1]).wait_send())
            pl.when(has_prev)(lambda: sent(2, comb).wait_send())

        return give, combine, total, drain

    v_give, v_combine, v_total, v_drain = backward("v", 1.0 / scale)
    k_give, k_combine, k_total, k_drain = backward("k", 1.0)

    vl = r["vl"]

    def low_swap(kv):
        return remote(
            vl.at[kv, pl.ds(0, T)],
            vl.at[kv, pl.ds(T, T)],
            r["vl_send"],
            r["vl_recv"].at[kv],
            node=partner,
        )

    @scoped("value_own")
    def value_own(kv):
        vl[kv, 0:T] = v_total(kv).astype(BF16)
        low_swap(kv).start()

    wacc, xk = r["wacc"], r["xk"]
    ys, yr, xs, xr, zs, zr = (r[k] for k in ("ys", "yr", "xs", "xr", "zs", "zr"))

    def y_copy(kv, h, s):
        return remote(
            ys.at[s - 1, kv, h],
            yr.at[L - s - 1, kv, h],
            r["y_send"].at[s - 1],
            r["y_recv"].at[L - s - 1, kv, h],
            local=lax.rem(l + s, L),
        )

    def x_copy(kv, h):
        return remote(xs.at[kv, h], xr.at[kv, h], r["x_send"], r["x_recv"].at[kv, h], node=xpeer)

    def z_copy(kv, s, h):
        there = lax.rem(z + s, NZ)
        return remote(
            zs.at[kv, h, lax.div(there, 2)],
            zr.at[NZ - s - 1, kv],
            r["z_send"].at[s - 1],
            r["z_recv"].at[NZ - s - 1, kv],
            node=lax.rem(n + 4 * s, N),
        )

    @scoped("terms")
    def grad_terms(kv):
        low_swap(kv).wait_recv()
        both = vl[kv]
        for h in range(2):
            for i in range(NZ // 2):
                for x in range(2):
                    j = (2 * i + h) * 2 + x
                    part = dot(hid_t[pl.ds(j * GW, GW)], both)
                    wacc[kv, j] = part.reshape(L, RO, C)
                    for s in range(1, L):
                        ys[s - 1, kv, h, i, x] = wacc[kv, j, lax.rem(l + s, L)].astype(BF16)
            for s in range(1, L):
                y_copy(kv, h, s).start()

    @scoped("second")
    def grad_second(kv, h):
        for s in range(1, L):
            y_copy(kv, h, L - s).wait_recv()

        def summed(i, x):
            total = wacc[kv, (2 * i + h) * 2 + x, l]
            for s in range(1, L):
                total = total + yr[s - 1, kv, h, i, x].astype(F32)
            return total

        for i in range(NZ // 2):
            xs[kv, h, i] = summed(i, 1 - xbit).astype(BF16)
        x_copy(kv, h).start()
        for i in range(NZ // 2):
            xk[kv, h, i] = summed(i, xbit)

    @scoped("third")
    def grad_third(kv, h):
        x_copy(kv, h).wait_recv()
        for i in range(NZ // 2):
            total = xk[kv, h, i] + xr[kv, h, i].astype(F32)
            xk[kv, h, i] = total
            zs[kv, h, i] = total.astype(BF16)
        for s in range(1, NZ):

            @pl.when(lax.rem(z + s, 2) == h)
            def _():
                z_copy(kv, s, h).start()

    @scoped("final")
    def grad_final(kv):
        for s in range(1, NZ):
            z_copy(kv, NZ - s, 0).wait_recv()
        total = xk[kv, zbit, lax.div(z, 2)]
        for s in range(1, NZ):
            total = total + zr[s - 1, kv].astype(F32)
        r["weight_grad"][kv] = total

    @scoped("key_own")
    def key_own(kv):
        r["key_grad"][kv] = k_total(kv).astype(BF16)

    probs, acc = r["probs"], r["acc"]

    def summed_into(first, part):
        if first:
            acc[...] = part
        else:
            acc[...] += part

    wide, slim, scaled = ((r[k + "_a"], r[k + "_b"]) for k in ("wide", "low", "gs"))
    width = DOCB * T
    piece = 8 * 16
    pieces = [slice(i, i + piece) for i in range(0, width, piece)]

    def eights(x, reduce):
        return reduce(x.reshape(x.shape[0] // 8, 8, x.shape[1]), axis=0)

    def at_rows(head):
        return pl.ds(head * T, T)

    def score_stage(kv, head):
        scores = dot_rows(kwin[kv], r["q"][kv, at_rows(head)])
        top = None
        for at_piece in pieces:
            beyond = r["outside"][at_piece]
            part = scores[at_piece] + jnp.concatenate([beyond] * (T // C), axis=1)
            if at_piece.start >= width - T:
                start = at_piece.start - (width - T)
                part = part + r["bias"][start : start + piece]
            wide[head % 2][at_piece] = part
            most = eights(part, jnp.max)
            top = most if top is None else jnp.maximum(top, most)
        return jnp.max(top, axis=0, keepdims=True)

    def softmax_stage(kv, head, top):
        total = None
        for at_piece in pieces:
            expd = jnp.exp2((wide[head % 2][at_piece] - top) * (scale * LOG2E))
            rounded = expd.astype(BF16)
            slim[head % 2][at_piece] = rounded
            probs[kv * G + head, at_piece] = rounded
            part = eights(expd, jnp.sum)
            total = part if total is None else total + part
        inverse = 1.0 / jnp.sum(total, axis=0, keepdims=True)
        r["inv"][kv * G + head] = inverse
        factor = jnp.broadcast_to(inverse * scale, (C, T)).T
        low_grad = (r["g"][kv, at_rows(head)].astype(F32) * factor).astype(BF16)
        scaled[head % 2][...] = low_grad
        r["gs"][kv, at_rows(head)] = low_grad

    def value_stage(kv, head):
        summed_into(head == 0, dot(slim[head % 2][...], scaled[head % 2][...]))

    def prob_stage(kv, head):
        prob_grad = dot_rows(vwin[kv], r["gs"][kv, at_rows(head)])
        total = None
        for at_piece in pieces:
            part = prob_grad[at_piece]
            wide[head % 2][at_piece] = part
            part = eights(part * probs[kv * G + head, at_piece].astype(F32), jnp.sum)
            total = part if total is None else total + part
        return jnp.sum(total, axis=0, keepdims=True) * r["inv"][kv * G + head]

    def score_grad_stage(kv, head, delta):
        for at_piece in pieces:
            p = probs[kv * G + head, at_piece].astype(F32)
            slim[head % 2][at_piece] = (p * (wide[head % 2][at_piece] - delta)).astype(BF16)

    def key_stage(kv, head):
        score_grad = slim[head % 2][...]
        query_grad = dot(kwin[kv].T, score_grad).T
        r["query_grad"][kv, :, head * C : (head + 1) * C] = query_grad.astype(BF16)
        summed_into(head == 0, dot(score_grad, r["q"][kv, at_rows(head)]))

    def staged(first, second, third):
        def early(kv):
            state = first(kv, 0)
            for head in range(half):
                following = first(kv, head + 1)
                second(kv, head, state)
                if head:
                    third(kv, head - 1)
                state = following
            return state

        def late(kv, state):
            for head in range(half, G):
                following = first(kv, head + 1) if head + 1 < G else None
                second(kv, head, state)
                third(kv, head - 1)
                state = following
            third(kv, G - 1)

        return early, late

    half = G // 2
    value_early, value_late = staged(score_stage, softmax_stage, value_stage)
    key_early, key_late = staged(prob_stage, score_grad_stage, key_stage)
    last = KVH - 1

    def at(kv, plan):
        for when_kv in sorted({k for k, *_ in plan}):

            @pl.when(kv == when_kv)
            def _():
                for k, task, *args in plan:
                    if k == when_kv:
                        task(*args)

    @scoped("partner_hid")
    def partner_hidden():
        hidden_all().wait_recv()
        for j in range(N // 2):
            hid_t[pl.ds(j * GW, GW), T : 2 * T] = hidp[j].T

    def more_keys(kv):
        key_in(kv).wait()
        key_start(kv)

    key_relay(0)
    for j in range(N // 2):
        hidden_swap(j).start()

    value_mid_plan = (
        [(kv, key_relay, kv + 1) for kv in range(KVH - 1)]
        + [(kv, v_combine, kv - 1) for kv in range(1, KVH)]
        + [(kv, weight_relay, kv) for kv in range(KVH)]
        + [(1, partner_hidden)]
        + [(2, weight_relay_again, 0)]
        + [(kv, value_own, kv - 2) for kv in range(2, KVH)]
    )
    value_end_plan = [(kv, grad_terms, kv - 2) for kv in range(2, KVH)]

    def value_pass(kv, carry):
        key_wait(kv)
        with jax.named_scope("value_early"):
            state = value_early(kv)
        at(kv, value_mid_plan)
        with jax.named_scope("value_late"):
            value_late(kv, state)
        v_give(kv, acc)
        at(kv, value_end_plan)
        return carry

    lax.fori_loop(0, KVH, value_pass, 0)

    weight_relay_again(1)
    v_combine(last)
    value_own(2)

    with jax.named_scope("weight_wait"):
        for s in range(1, L):
            for kind, index in weight_kinds:
                if kind >= 3:
                    weight_pass(s, index, kind).wait_recv()
    with jax.named_scope("rest_values"):
        values = r["vacc"][...]
        for s in range(1, L):
            there = pl.multiple_of(lax.rem(l + s, L) * R, R)
            values = values + dot(hid[:, pl.ds(there, R)], wfull[pl.ds(there, R)])
        for kv in range(KVH):
            vwin[kv, rows(0)] = values[:, kv * C : (kv + 1) * C].astype(BF16)
    for kv in range(KVH):
        value_start(kv)
    grad_terms(2)
    grad_second(0, 0)
    value_own(last)

    step = D // 8

    def input_passes(low, high):
        own_low = jnp.concatenate([vl[kv, 0:T] for kv in range(KVH)], axis=1)

        def input_pass(i, carry):
            at = pl.multiple_of(i * step, step)
            r["input_grad"][:, pl.ds(at, step)] = dot_rows(own_low, wfull[pl.ds(at, step)]).astype(BF16)
            return carry

        with jax.named_scope("input_grad"):
            lax.fori_loop(low, high, input_pass, 0)

    input_passes(0, 4)
    value_relay(0)
    grad_terms(last)
    grad_second(0, 1)

    key_mid_plan = (
        [(kv, value_relay, kv + 1) for kv in range(KVH - 1)]
        + [(kv, k_combine, kv - 1) for kv in range(1, KVH)]
        + [
            (0, grad_second, 1, 0),
            (2, grad_second, 3, 0),
            (1, grad_third, 0, 0),
            (1, grad_third, 0, 1),
            (2, grad_third, 1, 1),
            (2, grad_third, 2, 0),
            (3, grad_third, 3, 0),
        ]
    )
    key_end_plan = [
        (0, grad_second, 1, 1),
        (0, grad_second, 2, 0),
        (1, grad_second, 2, 1),
        (1, grad_third, 1, 0),
        (2, grad_second, 3, 1),
        (2, grad_third, 2, 1),
        (3, grad_third, 3, 1),
        (3, grad_final, 0),
    ] + [(kv, key_own, kv - 2) for kv in range(2, KVH)]

    def key_pass(kv, carry):
        value_wait(kv)
        with jax.named_scope("key_early"):
            state = key_early(kv)
        at(kv, key_mid_plan)
        with jax.named_scope("key_late"):
            key_late(kv, state)
        k_give(kv, acc)
        at(kv, key_end_plan)
        return carry

    lax.fori_loop(0, KVH, key_pass, 0)
    input_passes(4, 8)
    k_combine(last)
    grad_final(1)
    grad_final(2)
    key_own(last - 1)
    key_own(last)
    grad_final(last)

    for drain in (key_drain, value_drain, v_drain, k_drain):
        drain()
    remote(vl.at[:, 0:T], vl.at[:, 0:T], r["vl_send"], r["vl_recv"].at[0], node=partner).wait_send()
    for s in range(1, L):
        remote(
            ys.at[s - 1], ys.at[s - 1], r["y_send"].at[s - 1], r["y_recv"].at[0, 0, 0], node=partner
        ).wait_send()
        for kind in range(6):
            part = wfull.at[pl.ds(0, SUB * (4 if kind in (0, 3) else 2))]
            remote(
                part, part, r["w_send"].at[kind, s - 1], r["w_recv"].at[0, 0, 0], node=partner
            ).wait_send()
    remote(xs, xs, r["x_send"], r["x_recv"].at[0, 0], node=partner).wait_send()
    for s in range(1, NZ):
        part = zs.at[:, 0, 0]
        remote(
            part, part, r["z_send"].at[s - 1], r["z_recv"].at[0, 0], node=partner
        ).wait_send()
    hidden_all().wait_send()


def local(hidden, queries, saved_keys, grad_out, value_weight, doc_lengths, doc_order):
    N, L = lax.axis_size("node"), lax.axis_size("local")
    T, D = hidden.shape[1:]
    QW, KVW = queries.shape[2], saved_keys.shape[2]
    KVH = KVW // HD
    G = QW // KVW
    C = HD
    NZ, RO, GW, J = N // 4, D // (N * L), D // N, N // 2
    vmem = lambda *shape: lambda dtype: pltpu.VMEM(shape, dtype)
    dma = lambda *shape: pltpu.SemaphoreType.DMA(shape)
    scratch = dict(
        kwin=pltpu.VMEM((KVH, DOCB * T, C), BF16),
        vwin=pltpu.VMEM((KVH, DOCB * T, C), BF16),
        q=pltpu.VMEM((KVH, G * T, C), BF16),
        g=pltpu.VMEM((KVH, G * T, C), BF16),
        inv=pltpu.VMEM((KVH * G, 1, T), F32),
        outside=pltpu.VMEM((DOCB * T, C), F32),
        hid=pltpu.VMEM((T, D), BF16),
        hidp=pltpu.VMEM((J, T, GW), BF16),
        hid_t=pltpu.VMEM((J * GW, 2 * T), BF16),
        wfull=pltpu.VMEM((D, KVW), BF16),
        bias=pltpu.VMEM((T, T), F32),
        vacc=pltpu.VMEM((T, KVW), F32),
        probs=pltpu.VMEM((KVH * G, DOCB * T, T), BF16),
        wide_a=pltpu.VMEM((DOCB * T, T), F32),
        wide_b=pltpu.VMEM((DOCB * T, T), F32),
        low_a=pltpu.VMEM((DOCB * T, T), BF16),
        low_b=pltpu.VMEM((DOCB * T, T), BF16),
        gs_a=pltpu.VMEM((T, C), BF16),
        gs_b=pltpu.VMEM((T, C), BF16),
        gs=pltpu.VMEM((KVH, G * T, C), BF16),
        acc=pltpu.VMEM((DOCB * T, C), F32),
        vl=pltpu.VMEM((KVH, 2 * T, C), BF16),
        wacc=pltpu.VMEM((KVH, J, L, RO, C), F32),
        ys=pltpu.VMEM((L - 1, KVH, 2, NZ // 2, 2, RO, C), BF16),
        yr=pltpu.VMEM((L - 1, KVH, 2, NZ // 2, 2, RO, C), BF16),
        xs=pltpu.VMEM((KVH, 2, NZ // 2, RO, C), BF16),
        xr=pltpu.VMEM((KVH, 2, NZ // 2, RO, C), BF16),
        xk=pltpu.VMEM((KVH, 2, NZ // 2, RO, C), F32),
        zs=pltpu.VMEM((KVH, 2, NZ // 2, RO, C), BF16),
        zr=pltpu.VMEM((NZ - 1, KVH, RO, C), BF16),
        key_in_sem=dma(KVH),
        query_in_sem=dma(KVH),
        grad_in_sem=dma(KVH),
        in_sem=dma(2),
        w_send=dma(6, L - 1),
        w_recv=dma(6, L - 1, 4),
        h_send=pltpu.SemaphoreType.DMA,
        h_recv=pltpu.SemaphoreType.DMA,
        vl_send=pltpu.SemaphoreType.DMA,
        vl_recv=dma(KVH),
        y_send=dma(L - 1),
        y_recv=dma(L - 1, KVH, 2),
        x_send=pltpu.SemaphoreType.DMA,
        x_recv=dma(KVH, 2),
        z_send=dma(NZ - 1),
        z_recv=dma(NZ - 1, KVH),
    )
    for name in ("kw", "vw", "v", "k"):
        scratch[name + "_send"] = dma(3)
        scratch[name + "_recv"] = dma(3, KVH)
    for name in ("v", "k"):
        scratch[name + "_out"] = pltpu.VMEM((KVH, 2, T, C), BF16)
        for extra in ("_mid", "_comb", "_near", "_third"):
            scratch[name + extra] = pltpu.VMEM((KVH, T, C), BF16)
        for extra in ("_own", "_keep"):
            scratch[name + extra] = pltpu.VMEM((KVH, T, C), F32)
    args = ("lengths", "order", "hidden", "queries", "keys", "grads", "weight")
    outs = ("query_grad", "key_grad", "input_grad", "weight_grad")
    sizes = dict(N=N, L=L, T=T, D=D, KVH=KVH, G=G, names=args + outs + tuple(scratch))
    smem = pl.BlockSpec(memory_space=pltpu.SMEM)
    anywhere = pl.BlockSpec(memory_space=pltpu.HBM)
    held = pl.BlockSpec(memory_space=pltpu.VMEM)
    grads = pl.pallas_call(
        functools.partial(kernel, sizes),
        out_shape=[
            pltpu.VMEM((KVH, T, G * C), BF16),
            pltpu.VMEM((KVH, T, C), BF16),
            pltpu.VMEM((T, D), BF16),
            pltpu.VMEM((KVH, RO, C), F32),
        ],
        in_specs=[smem, smem] + [anywhere] * 5,
        out_specs=[held] * 4,
        scratch_shapes=list(scratch.values()),
        compiler_params=pltpu.CompilerParams(
            collective_id=0, has_side_effects=True, vmem_limit_bytes=60 * 2**20
        ),
        name="attention_grads",
    )(
        doc_lengths,
        doc_order,
        hidden[0],
        queries[0],
        saved_keys[0],
        grad_out[0],
        value_weight,
    )
    return results(
        grads,
        [
            jax.ShapeDtypeStruct((1, T, QW), BF16),
            jax.ShapeDtypeStruct((1, T, KVW), BF16),
            jax.ShapeDtypeStruct((1, T, D), BF16),
            jax.ShapeDtypeStruct((RO, KVW), F32),
        ],
    )


def results_kernel(query_in, key_in, input_in, weight_in, query, key, x, weight, sems):
    copies = [(input_in, x.at[0])]
    for kv in range(query_in.shape[0]):
        for a, b in ((query_in, query.at[0]), (key_in, key.at[0]), (weight_in, weight)):
            width = a.shape[2]
            copies.append((a.at[kv], b.at[:, pl.ds(kv * width, width)]))
    copies = [pltpu.make_async_copy(a, b, sems.at[i]) for i, (a, b) in enumerate(copies)]
    for copy in copies:
        copy.start()
    for copy in copies:
        copy.wait()


def results(arrays, shapes):
    heads = arrays[0].shape[0]
    return pl.pallas_call(
        results_kernel,
        out_shape=shapes,
        in_specs=[pl.BlockSpec(memory_space=pltpu.VMEM)] * len(arrays),
        out_specs=[pl.BlockSpec(memory_space=pl.ANY)] * len(arrays),
        scratch_shapes=[pltpu.SemaphoreType.DMA((1 + 3 * heads,))],
        compiler_params=pltpu.CompilerParams(vmem_limit_bytes=2**20),
        name="results",
    )(*arrays)


def solution(mesh):
    tokens = P("local", "node", None)
    return jax.shard_map(
        local,
        mesh=mesh,
        in_specs=(tokens,) * 4 + (P("local", None),) * 3,
        out_specs=(tokens,) * 3 + (P(("node", "local"), None),),
        check_vma=False,
    )
```

```python
import functools

import jax
import jax.numpy as jnp
from jax import lax
from jax.experimental import pallas as pl
from jax.experimental.pallas import tpu as pltpu
from jax.sharding import PartitionSpec as P

HD = 128
DOCB = 4
BF16 = jnp.bfloat16
F32 = jnp.float32
LOG2E = 1.4426950408889634
MESH = pl.DeviceIdType.MESH

masked_score = -1e30

ROWS_BY_ROWS = (((1,), (1,)), ((), ()))


def dot(a, b):
    return jnp.dot(a, b, preferred_element_type=F32)


def dot_rows(a, b):
    return lax.dot_general(a, b, ROWS_BY_ROWS, preferred_element_type=F32)


def remote(src, dst, send_sem, recv_sem, **where):
    return pltpu.make_async_remote_copy(
        src_ref=src,
        dst_ref=dst,
        send_sem=send_sem,
        recv_sem=recv_sem,
        device_id=where,
        device_id_type=MESH,
    )


def scoped(name):
    def wrap(function):
        @functools.wraps(function)
        def inner(*args):
            with jax.named_scope(name):
                return function(*args)

        return inner

    return wrap


def kernel(sizes, *refs):
    N, L, T, D, KVH, G = (sizes[k] for k in ("N", "L", "T", "D", "KVH", "G"))
    names = sizes["names"]
    r = dict(zip(names, refs))
    C = HD
    NZ = N // 4
    RO = D // (N * L)
    GW = D // N
    R = D // L
    QUARTER, SUB = R // 4, R // 16
    GC = G * C
    scale = HD ** (-0.5)

    n = lax.axis_index("node")
    l = lax.axis_index("local")
    core = lax.rem(n, 2)
    even, odd = core == 0, core == 1
    partner = n + 1 - 2 * core
    xbit = lax.rem(lax.div(n, 2), 2)
    xpeer = n + 2 - 4 * xbit
    z = lax.div(n, 4)
    zbit = lax.rem(z, 2)
    zpeer = n + 4 - 8 * zbit
    has_next, has_prev = n + 2 < N, n >= 2
    has_far_next, has_far_prev = n + 3 < N, n >= 3

    kwin, vwin = r["kwin"], r["vwin"]
    hid, hidp, hid_t, wfull = r["hid"], r["hidp"], r["hid_t"], r["wfull"]

    def rows(offset):
        return pl.ds((DOCB - 1 - offset) * T, T)

    for offset in range(1, DOCB):

        @pl.when(n < offset)
        def _():
            for win in (kwin, vwin):
                for kv in range(KVH):
                    win[kv, rows(offset)] = jnp.zeros((T, C), BF16)

    for name in ("v", "k"):

        @pl.when(n + 2 >= N)
        def _():
            r[name + "_near"][...] = jnp.zeros((KVH, T, C), BF16)

        @pl.when(jnp.logical_and(odd, n + 3 >= N))
        def _():
            r[name + "_third"][...] = jnp.zeros((KVH, T, C), BF16)

    def local_copy(src, dst, sem):
        return pltpu.make_async_copy(src, dst, sem)

    def key_in(kv):
        return local_copy(
            r["keys"].at[:, pl.ds(kv * C, C)], kwin.at[kv, rows(0)], r["key_in_sem"].at[kv]
        )

    def head_copies(source, into, sem, kv):
        return [
            local_copy(
                r[source].at[:, pl.ds(kv * GC + head * C, C)],
                r[into].at[kv, pl.ds(head * T, T)],
                r[sem],
            )
            for head in range(G)
        ]

    def heads_wait(into, sem):
        local_copy(r[into], r[into], r[sem]).wait()

    hidden_in = local_copy(r["hidden"], hid, r["in_sem"].at[0])
    weight_in = local_copy(r["weight"], wfull.at[pl.ds(l * R, R)], r["in_sem"].at[1])
    for kv in range(KVH):
        key_in(kv).start()
    hidden_in.start()
    weight_in.start()
    for kv in range(KVH):
        for copy in head_copies("queries", "q", "query_in_sem", kv):
            copy.start()
        for copy in head_copies("grads", "g", "grad_in_sem", kv):
            copy.start()

    barrier = pltpu.get_barrier_semaphore()

    def greet(**where):
        pl.semaphore_signal(barrier, inc=1, device_id=where, device_id_type=MESH)

    greet(node=partner)
    for there, who in (
        (has_next, n + 2),
        (has_prev, n - 2),
        (jnp.logical_and(odd, has_far_next), n + 3),
        (jnp.logical_and(even, has_far_prev), n - 3),
    ):

        @pl.when(there)
        def _():
            greet(node=who)

    for s in range(1, L):
        greet(local=lax.rem(l + s, L))
    for s in range(1, NZ):
        greet(node=lax.rem(n + 4 * s, N))
    as_int = lambda b: jnp.where(b, 1, 0)
    expected = (
        1
        + as_int(has_next)
        + as_int(has_prev)
        + core * as_int(has_far_next)
        + (1 - core) * as_int(has_far_prev)
        + (L - 1)
        + (NZ - 1)
    )
    with jax.named_scope("entry"):
        pl.semaphore_wait(barrier, expected)

    def window(win, name):
        send, recv = r[name + "_send"], r[name + "_recv"]

        def ahead(kv):
            return remote(
                win.at[kv, rows(0)], win.at[kv, rows(2)], send.at[0], recv.at[1, kv], node=n + 2
            )

        def beside(kv):
            return remote(
                win.at[kv, rows(0)], win.at[kv, rows(1)], send.at[1], recv.at[0, kv], node=n + 1
            )

        def far(kv):
            return remote(
                win.at[kv, rows(0)], win.at[kv, rows(3)], send.at[1], recv.at[2, kv], node=n + 3
            )

        def relay_even(kv):
            return remote(
                win.at[kv, rows(2)], win.at[kv, rows(3)], send.at[2], recv.at[2, kv], node=n + 1
            )

        def relay_odd(kv):
            return remote(
                win.at[kv, rows(2)], win.at[kv, rows(1)], send.at[2], recv.at[0, kv], node=n - 1
            )

        far_there = jnp.logical_and(odd, has_far_next)
        relay_e = jnp.logical_and(even, has_prev)
        relay_o = jnp.logical_and(odd, has_prev)

        @scoped(name + "_start")
        def start(kv):
            pl.when(has_next)(lambda: ahead(kv).start())
            pl.when(far_there)(lambda: far(kv).start())
            pl.when(even)(lambda: beside(kv).start())

        @scoped(name + "_relay")
        def relay(kv):
            @pl.when(has_prev)
            def _():
                ahead(kv).wait_recv()

            pl.when(relay_e)(lambda: relay_even(kv).start())
            pl.when(relay_o)(lambda: relay_odd(kv).start())

        @scoped(name + "_wait")
        def wait(kv):
            pl.when(jnp.logical_or(odd, has_prev))(lambda: beside(kv).wait_recv())
            pl.when(has_far_prev)(lambda: far(kv).wait_recv())

        def drain():
            def sent(kind, place):
                part = win.at[:, rows(place)]
                return remote(part, part, send.at[kind], recv.at[0, 0], node=partner)

            pl.when(has_next)(lambda: sent(0, 0).wait_send())
            pl.when(jnp.logical_or(even, has_far_next))(lambda: sent(1, 0).wait_send())
            pl.when(has_prev)(lambda: sent(2, 2).wait_send())

        return start, relay, wait, drain

    key_start, key_relay, key_wait, key_drain = window(kwin, "kw")
    value_start, value_relay, value_wait, value_drain = window(vwin, "vw")

    for kv in range(KVH):
        key_in(kv).wait()
        key_start(kv)

    def weight_part(owner, zb, xb, sub):
        return pl.ds(owner * R + (zb * 2 + xb) * QUARTER + (core * 2 + sub) * SUB, SUB)

    def weight_class(owner, index):
        if index < 2:
            return weight_part(owner, zbit, xbit, index)
        return weight_part(owner, 1 - zbit, 1 - xbit, index - 2)

    def weight_start(s, index):
        return remote(
            r["weight"].at[weight_class(0, index)],
            wfull.at[weight_class(l, index)],
            r["w_send"].at[0, s - 1],
            r["w_recv"].at[0, L - s - 1, index],
            local=lax.rem(l + s, L),
        )

    def weight_pass(s, index, kind):
        owner = lax.rem(l + s, L)
        if kind <= 3:
            rows_at = weight_class(owner, index)
        elif kind == 4:
            rows_at = weight_part(owner, 1 - zbit, xbit, index)
        else:
            rows_at = weight_part(owner, zbit, 1 - xbit, index)
        part = wfull.at[rows_at]
        return remote(
            part,
            part,
            r["w_send"].at[kind, s - 1],
            r["w_side"] if kind >= 3 else r["w_recv"].at[kind, s - 1, index],
            node={1: zpeer, 2: xpeer}.get(kind, partner),
        )

    @scoped("weight_relay")
    def weight_relay(index):
        for s in range(1, L):
            weight_start(L - s, index).wait_recv()
            if index < 2:
                weight_pass(s, index, 1).start()
                weight_pass(s, index, 2).start()
            weight_pass(s, index, 3).start()

    @scoped("weight_again")
    def weight_relay_again(sub):
        for s in range(1, L):
            weight_pass(s, sub, 1).wait_recv()
            weight_pass(s, sub, 4).start()
            weight_pass(s, sub, 2).wait_recv()
            weight_pass(s, sub, 5).start()

    weight_kinds = [(k, i) for k in (3, 1, 2, 4, 5) for i in range(4) if k == 3 or i < 2]

    for sub in range(4):
        for s in range(1, L):
            weight_start(s, sub).start()

    def hidden_swap(j):
        cols = pl.ds((2 * j + 1 - core) * GW, GW)
        return remote(
            r["hidden"].at[:, cols], hidp.at[j], r["h_send"], r["h_recv"], node=partner
        )

    def hidden_all():
        return remote(hidp, hidp, r["h_send"], r["h_recv"], node=partner)

    block = n

    def find(j, carry):
        first, start, length = carry
        size = r["lengths"][0, r["order"][0, j]]
        count = lax.div(size + (T - 1), T)
        inside = jnp.logical_and(first <= block, block < first + count)
        return (
            first + count,
            jnp.where(inside, first, start),
            jnp.where(inside, size, length),
        )

    zero = jnp.int32(0)
    _, doc_start, doc_length = lax.fori_loop(0, r["lengths"].shape[1], find, (zero, zero, zero))
    low = (doc_start - block + (DOCB - 1)) * T
    high = low + doc_length
    key_at = lax.broadcasted_iota(jnp.int32, (DOCB * T, C), 0)
    outside = jnp.logical_or(key_at < low, key_at >= high)
    r["outside"][...] = jnp.where(outside, masked_score, 0.0)
    later = lax.broadcasted_iota(jnp.int32, (T, T), 0) > lax.broadcasted_iota(jnp.int32, (T, T), 1)
    r["bias"][...] = jnp.where(later, masked_score, 0.0)
    query_row = lax.broadcasted_iota(jnp.int32, (T, C), 0) + (DOCB - 1) * T
    query_ok = query_row < high

    with jax.named_scope("hid_in"):
        hidden_in.wait()
    weight_in.wait()
    with jax.named_scope("turn_hid"):
      for j in range(N // 2):
        cols = pl.ds(pl.multiple_of((2 * j + core) * GW, GW), GW)
        hid_t[pl.ds(j * GW, GW), 0:T] = hid[:, cols].T
    own_cols = pl.ds(pl.multiple_of(l * R, R), R)
    with jax.named_scope("half_values"):
        r["vacc"][...] = dot(hid[:, own_cols], wfull[pl.ds(pl.multiple_of(l * R, R), R)])
    heads_wait("q", "query_in_sem")
    heads_wait("g", "grad_in_sem")
    with jax.named_scope("mask_g"):
      for kv in range(KVH):
        for head in range(G):
            at_rows = pl.ds(head * T, T)
            masked = jnp.where(query_ok, r["g"][kv, at_rows].astype(F32), 0.0)
            r["g"][kv, at_rows] = masked.astype(BF16)

    def backward(name, factor):
        send, recv = r[name + "_send"], r[name + "_recv"]
        out, mid, comb = r[name + "_out"], r[name + "_mid"], r[name + "_comb"]
        near, third, own, keep = (r[name + e] for e in ("_near", "_third", "_own", "_keep"))
        to_third = jnp.logical_or(odd, has_far_prev)
        third_node = jnp.where(even, n - 3, n - 1)
        from_third = jnp.logical_or(even, has_far_next)

        def across(kv):
            return remote(out.at[kv, 0], mid.at[kv], send.at[0], recv.at[0, kv], node=partner)

        def skip(kv):
            return remote(
                out.at[kv, 1], third.at[kv], send.at[1], recv.at[1, kv], node=third_node
            )

        def back(kv):
            return remote(comb.at[kv], near.at[kv], send.at[2], recv.at[2, kv], node=n - 2)

        @scoped(name + "_give")
        def give(kv, acc):
            out[kv, 0] = (acc[pl.ds((1 - core) * 2 * T, T)] * factor).astype(BF16)
            out[kv, 1] = (acc[pl.ds(core * 2 * T, T)] * factor).astype(BF16)
            across(kv).start()
            pl.when(to_third)(lambda: skip(kv).start())
            keep[kv] = acc[rows(2)] * factor
            own[kv] = acc[rows(0)] * factor

        @scoped(name + "_combine")
        def combine(kv):
            across(kv).wait_recv()

            @pl.when(has_prev)
            def _():
                comb[kv] = (keep[kv] + mid[kv].astype(F32)).astype(BF16)
                back(kv).start()

        def total(kv):
            pl.when(from_third)(lambda: skip(kv).wait_recv())
            pl.when(has_next)(lambda: back(kv).wait_recv())
            return own[kv] + near[kv].astype(F32) + third[kv].astype(F32)

        def drain():
            def sent(kind, part):
                return remote(part, part, send.at[kind], recv.at[0, 0], node=partner)

            sent(0, out.at[:, 0]).wait_send()
            pl.when(to_third)(lambda: sent(1, out.at[:, 1]).wait_send())
            pl.when(has_prev)(lambda: sent(2, comb).wait_send())

        return give, combine, total, drain

    v_give, v_combine, v_total, v_drain = backward("v", 1.0 / scale)
    k_give, k_combine, k_total, k_drain = backward("k", 1.0)

    vl = r["vl"]

    def low_swap(kv):
        return remote(
            vl.at[kv, pl.ds(0, T)],
            vl.at[kv, pl.ds(T, T)],
            r["vl_send"],
            r["vl_recv"].at[kv],
            node=partner,
        )

    @scoped("value_own")
    def value_own(kv):
        vl[kv, 0:T] = v_total(kv).astype(BF16)
        low_swap(kv).start()

    wacc, xk = r["wacc"], r["xk"]
    ys, yr, xs, xr, zs, zr = (r[k] for k in ("ys", "yr", "xs", "xr", "zs", "zr"))

    def y_copy(kv, h, s):
        return remote(
            ys.at[s - 1, kv, h],
            yr.at[L - s - 1, kv, h],
            r["y_send"].at[s - 1],
            r["y_recv"].at[L - s - 1, kv, h],
            local=lax.rem(l + s, L),
        )

    def x_copy(kv, h):
        return remote(xs.at[kv, h], xr.at[kv, h], r["x_send"], r["x_recv"].at[kv, h], node=xpeer)

    def z_copy(kv, s, h):
        there = lax.rem(z + s, NZ)
        return remote(
            zs.at[kv, h, lax.rem(there, NZ // 2)],
            zr.at[kv, NZ - s - 1],
            r["z_send"].at[s - 1],
            r["z_recv"].at[kv],
            node=lax.rem(n + 4 * s, N),
        )

    @scoped("terms")
    def grad_terms(kv):
        low_swap(kv).wait_recv()
        both = vl[kv]
        for h in range(2):
            for i in range(NZ // 2):
                for x in range(2):
                    j = (h * (NZ // 2) + i) * 2 + x
                    part = dot(hid_t[pl.ds(j * GW, GW)], both)
                    wacc[kv, j] = part.reshape(L, RO, C)
                    for s in range(1, L):
                        ys[s - 1, kv, h, i, x] = wacc[kv, j, lax.rem(l + s, L)].astype(BF16)
            for s in range(1, L):
                y_copy(kv, h, s).start()

    @scoped("second")
    def grad_second(kv, h):
        for s in range(1, L):
            y_copy(kv, h, L - s).wait_recv()

        def summed(i, x):
            total = wacc[kv, (h * (NZ // 2) + i) * 2 + x, l]
            for s in range(1, L):
                total = total + yr[s - 1, kv, h, i, x].astype(F32)
            return total

        for i in range(NZ // 2):
            xs[kv, h, i] = summed(i, 1 - xbit).astype(BF16)
        x_copy(kv, h).start()
        for i in range(NZ // 2):
            xk[kv, h, i] = summed(i, xbit)

    @scoped("third")
    def grad_third(kv, h):
        x_copy(kv, h).wait_recv()
        for i in range(NZ // 2):
            total = xk[kv, h, i] + xr[kv, h, i].astype(F32)
            xk[kv, h, i] = total
            zs[kv, h, i] = total.astype(BF16)
        for s in range(1, NZ):

            @pl.when(lax.div(lax.rem(z + s, NZ), NZ // 2) == h)
            def _():
                z_copy(kv, s, h).start()

    @scoped("final")
    def grad_final(kv):
        remote(zr.at[kv], zr.at[kv], r["z_send"].at[0], r["z_recv"].at[kv], node=partner).wait_recv()
        total = xk[kv, lax.div(z, NZ // 2), lax.rem(z, NZ // 2)]
        for s in range(1, NZ):
            total = total + zr[kv, s - 1].astype(F32)
        r["weight_grad"][kv] = total

    @scoped("key_own")
    def key_own(kv):
        r["key_grad"][kv] = k_total(kv).astype(BF16)

    probs, acc = r["probs"], r["acc"]

    def summed_into(first, part):
        if first:
            acc[...] = part
        else:
            acc[...] += part

    wide, slim, scaled = ((r[k + "_a"], r[k + "_b"]) for k in ("wide", "low", "gs"))
    width = DOCB * T
    piece = 8 * 16
    pieces = [slice(i, i + piece) for i in range(0, width, piece)]

    def eights(x, reduce):
        return reduce(x.reshape(x.shape[0] // 8, 8, x.shape[1]), axis=0)

    def at_rows(head):
        return pl.ds(head * T, T)

    def score_stage(kv, head):
        scores = dot_rows(kwin[kv], r["q"][kv, at_rows(head)])
        top = None
        for at_piece in pieces:
            beyond = r["outside"][at_piece]
            part = scores[at_piece] + jnp.concatenate([beyond] * (T // C), axis=1)
            if at_piece.start >= width - T:
                start = at_piece.start - (width - T)
                part = part + r["bias"][start : start + piece]
            wide[head % 2][at_piece] = part
            most = eights(part, jnp.max)
            top = most if top is None else jnp.maximum(top, most)
        return jnp.max(top, axis=0, keepdims=True)

    def softmax_stage(kv, head, top):
        total = None
        for at_piece in pieces:
            expd = jnp.exp2((wide[head % 2][at_piece] - top) * (scale * LOG2E))
            rounded = expd.astype(BF16)
            slim[head % 2][at_piece] = rounded
            probs[kv * G + head, at_piece] = rounded
            part = eights(expd, jnp.sum)
            total = part if total is None else total + part
        inverse = 1.0 / jnp.sum(total, axis=0, keepdims=True)
        r["inv"][kv * G + head] = inverse
        factor = jnp.broadcast_to(inverse * scale, (C, T)).T
        low_grad = (r["g"][kv, at_rows(head)].astype(F32) * factor).astype(BF16)
        scaled[head % 2][...] = low_grad
        r["gs"][kv, at_rows(head)] = low_grad

    def value_stage(kv, head):
        summed_into(head == 0, dot(slim[head % 2][...], scaled[head % 2][...]))

    def prob_stage(kv, head):
        prob_grad = dot_rows(vwin[kv], r["gs"][kv, at_rows(head)])
        total = None
        for at_piece in pieces:
            part = prob_grad[at_piece]
            wide[head % 2][at_piece] = part
            part = eights(part * probs[kv * G + head, at_piece].astype(F32), jnp.sum)
            total = part if total is None else total + part
        return jnp.sum(total, axis=0, keepdims=True) * r["inv"][kv * G + head]

    def score_grad_stage(kv, head, delta):
        for at_piece in pieces:
            p = probs[kv * G + head, at_piece].astype(F32)
            slim[head % 2][at_piece] = (p * (wide[head % 2][at_piece] - delta)).astype(BF16)

    def key_stage(kv, head):
        score_grad = slim[head % 2][...]
        query_grad = dot(kwin[kv].T, score_grad).T
        r["query_grad"][kv, :, head * C : (head + 1) * C] = query_grad.astype(BF16)
        summed_into(head == 0, dot(score_grad, r["q"][kv, at_rows(head)]))

    def staged(first, second, third):
        def early(kv):
            state = first(kv, 0)
            for head in range(half):
                following = first(kv, head + 1)
                second(kv, head, state)
                if head:
                    third(kv, head - 1)
                state = following
            return state

        def late(kv, state):
            for head in range(half, G):
                following = first(kv, head + 1) if head + 1 < G else None
                second(kv, head, state)
                third(kv, head - 1)
                state = following
            third(kv, G - 1)

        return early, late

    half = G // 2
    value_early, value_late = staged(score_stage, softmax_stage, value_stage)
    key_early, key_late = staged(prob_stage, score_grad_stage, key_stage)
    last = KVH - 1

    def at(kv, plan):
        for when_kv in sorted({k for k, *_ in plan}):

            @pl.when(kv == when_kv)
            def _():
                for k, task, *args in plan:
                    if k == when_kv:
                        task(*args)

    @scoped("partner_hid")
    def partner_hidden():
        hidden_all().wait_recv()
        for j in range(N // 2):
            hid_t[pl.ds(j * GW, GW), T : 2 * T] = hidp[j].T

    def more_keys(kv):
        key_in(kv).wait()
        key_start(kv)

    key_relay(0)
    for j in range(N // 2):
        hidden_swap(j).start()

    def make_values():
        with jax.named_scope("weight_wait"):
            part = wfull.at[pl.ds(0, (L - 1) * R // 2)]
            remote(part, part, r["w_send"].at[0, 0], r["w_side"], node=partner).wait_recv()
        with jax.named_scope("rest_values"):
            values = r["vacc"][...]
            for s in range(1, L):
                there = pl.multiple_of(lax.rem(l + s, L) * R, R)
                values = values + dot(hid[:, pl.ds(there, R)], wfull[pl.ds(there, R)])
            for kv in range(KVH):
                vwin[kv, rows(0)] = values[:, kv * C : (kv + 1) * C].astype(BF16)
        for kv in range(KVH):
            value_start(kv)

    step = D // 8

    def input_passes(low, high):
        own_low = jnp.concatenate([vl[kv, 0:T] for kv in range(KVH)], axis=1)

        def input_pass(i, carry):
            at = pl.multiple_of(i * step, step)
            r["input_grad"][:, pl.ds(at, step)] = dot_rows(own_low, wfull[pl.ds(at, step)]).astype(BF16)
            return carry

        with jax.named_scope("input_grad"):
            lax.fori_loop(low, high, input_pass, 0)

    def input_part(i):
        input_passes(2 * i, 2 * i + 2)

    value_mid_plan = [
        (0, key_relay, 1),
        (0, weight_relay, 0),
        (1, key_relay, 2),
        (1, v_combine, 0),
        (1, weight_relay, 1),
        (1, partner_hidden),
        (2, key_relay, 3),
        (2, v_combine, 1),
        (2, weight_relay, 2),
        (2, weight_relay_again, 0),
        (2, value_own, 0),
        (3, v_combine, 2),
        (3, weight_relay, 3),
        (3, value_own, 1),
    ]
    value_end_plan = [
        (2, grad_terms, 0),
    ]

    def value_pass(kv, carry):
        key_wait(kv)
        with jax.named_scope("value_early"):
            state = value_early(kv)
        at(kv, value_mid_plan)
        with jax.named_scope("value_late"):
            value_late(kv, state)
        v_give(kv, acc)
        at(kv, value_end_plan)
        return carry

    lax.fori_loop(0, KVH, value_pass, 0)

    grad_terms(1)
    weight_relay_again(1)
    v_combine(3)
    value_own(2)
    make_values()
    grad_terms(2)
    value_own(3)
    input_part(0)
    grad_second(0, 0)
    input_part(1)
    value_relay(0)
    grad_terms(3)
    grad_second(0, 1)

    key_mid_plan = [
        (0, value_relay, 1),
        (0, grad_second, 1, 0),
        (1, value_relay, 2),
        (1, k_combine, 0),
        (1, grad_second, 2, 0),
        (1, grad_third, 0, 0),
        (1, grad_third, 0, 1),
        (2, k_combine, 1),
        (2, value_relay, 3),
        (2, grad_second, 3, 0),
        (2, grad_third, 1, 1),
        (2, grad_third, 2, 0),
        (3, grad_third, 3, 0),
        (3, grad_second, 3, 1),
        (3, k_combine, 2),
    ]
    key_end_plan = [
        (0, grad_second, 1, 1),
        (1, grad_second, 2, 1),
        (1, grad_third, 1, 0),
        (2, grad_third, 2, 1),
        (2, key_own, 0),
    ]

    def key_pass(kv, carry):
        value_wait(kv)
        with jax.named_scope("key_early"):
            state = key_early(kv)
        at(kv, key_mid_plan)
        with jax.named_scope("key_late"):
            key_late(kv, state)
        k_give(kv, acc)
        at(kv, key_end_plan)
        return carry

    lax.fori_loop(0, KVH, key_pass, 0)

    grad_third(3, 1)
    grad_final(0)
    k_combine(3)
    input_part(2)
    key_own(1)
    input_part(3)
    grad_final(1)
    grad_final(2)
    key_own(2)
    key_own(3)
    grad_final(3)

    for drain in (key_drain, value_drain, v_drain, k_drain):
        drain()
    remote(vl.at[:, 0:T], vl.at[:, 0:T], r["vl_send"], r["vl_recv"].at[0], node=partner).wait_send()
    for s in range(1, L):
        remote(
            ys.at[s - 1], ys.at[s - 1], r["y_send"].at[s - 1], r["y_recv"].at[0, 0, 0], node=partner
        ).wait_send()
        for kind in range(6):
            part = wfull.at[pl.ds(0, SUB * (4 if kind in (0, 3) else 2))]
            remote(
                part, part, r["w_send"].at[kind, s - 1], r["w_recv"].at[0, 0, 0], node=partner
            ).wait_send()
    remote(xs, xs, r["x_send"], r["x_recv"].at[0, 0], node=partner).wait_send()
    for s in range(1, NZ):
        part = zs.at[:, 0, 0]
        remote(
            part, part, r["z_send"].at[s - 1], r["z_recv"].at[0], node=partner
        ).wait_send()
    hidden_all().wait_send()


def local(hidden, queries, saved_keys, grad_out, value_weight, doc_lengths, doc_order):
    N, L = lax.axis_size("node"), lax.axis_size("local")
    T, D = hidden.shape[1:]
    QW, KVW = queries.shape[2], saved_keys.shape[2]
    KVH = KVW // HD
    G = QW // KVW
    C = HD
    NZ, RO, GW, J = N // 4, D // (N * L), D // N, N // 2
    vmem = lambda *shape: lambda dtype: pltpu.VMEM(shape, dtype)
    dma = lambda *shape: pltpu.SemaphoreType.DMA(shape)
    scratch = dict(
        kwin=pltpu.VMEM((KVH, DOCB * T, C), BF16),
        vwin=pltpu.VMEM((KVH, DOCB * T, C), BF16),
        q=pltpu.VMEM((KVH, G * T, C), BF16),
        g=pltpu.VMEM((KVH, G * T, C), BF16),
        inv=pltpu.VMEM((KVH * G, 1, T), F32),
        outside=pltpu.VMEM((DOCB * T, C), F32),
        hid=pltpu.VMEM((T, D), BF16),
        hidp=pltpu.VMEM((J, T, GW), BF16),
        hid_t=pltpu.VMEM((J * GW, 2 * T), BF16),
        wfull=pltpu.VMEM((D, KVW), BF16),
        bias=pltpu.VMEM((T, T), F32),
        vacc=pltpu.VMEM((T, KVW), F32),
        probs=pltpu.VMEM((KVH * G, DOCB * T, T), BF16),
        wide_a=pltpu.VMEM((DOCB * T, T), F32),
        wide_b=pltpu.VMEM((DOCB * T, T), F32),
        low_a=pltpu.VMEM((DOCB * T, T), BF16),
        low_b=pltpu.VMEM((DOCB * T, T), BF16),
        gs_a=pltpu.VMEM((T, C), BF16),
        gs_b=pltpu.VMEM((T, C), BF16),
        gs=pltpu.VMEM((KVH, G * T, C), BF16),
        acc=pltpu.VMEM((DOCB * T, C), F32),
        vl=pltpu.VMEM((KVH, 2 * T, C), BF16),
        wacc=pltpu.VMEM((KVH, J, L, RO, C), F32),
        ys=pltpu.VMEM((L - 1, KVH, 2, NZ // 2, 2, RO, C), BF16),
        yr=pltpu.VMEM((L - 1, KVH, 2, NZ // 2, 2, RO, C), BF16),
        xs=pltpu.VMEM((KVH, 2, NZ // 2, RO, C), BF16),
        xr=pltpu.VMEM((KVH, 2, NZ // 2, RO, C), BF16),
        xk=pltpu.VMEM((KVH, 2, NZ // 2, RO, C), F32),
        zs=pltpu.VMEM((KVH, 2, NZ // 2, RO, C), BF16),
        zr=pltpu.VMEM((KVH, NZ - 1, RO, C), BF16),
        key_in_sem=dma(KVH),
        query_in_sem=pltpu.SemaphoreType.DMA,
        grad_in_sem=pltpu.SemaphoreType.DMA,
        in_sem=dma(2),
        w_send=dma(6, L - 1),
        w_recv=dma(3, L - 1, 4),
        w_side=pltpu.SemaphoreType.DMA,
        h_send=pltpu.SemaphoreType.DMA,
        h_recv=pltpu.SemaphoreType.DMA,
        vl_send=pltpu.SemaphoreType.DMA,
        vl_recv=dma(KVH),
        y_send=dma(L - 1),
        y_recv=dma(L - 1, KVH, 2),
        x_send=pltpu.SemaphoreType.DMA,
        x_recv=dma(KVH, 2),
        z_send=dma(NZ - 1),
        z_recv=dma(KVH),
    )
    for name in ("kw", "vw", "v", "k"):
        scratch[name + "_send"] = dma(3)
        scratch[name + "_recv"] = dma(3, KVH)
    for name in ("v", "k"):
        scratch[name + "_out"] = pltpu.VMEM((KVH, 2, T, C), BF16)
        for extra in ("_mid", "_comb", "_near", "_third"):
            scratch[name + extra] = pltpu.VMEM((KVH, T, C), BF16)
        for extra in ("_own", "_keep"):
            scratch[name + extra] = pltpu.VMEM((KVH, T, C), F32)
    args = ("lengths", "order", "hidden", "queries", "keys", "grads", "weight")
    outs = ("query_grad", "key_grad", "input_grad", "weight_grad")
    sizes = dict(N=N, L=L, T=T, D=D, KVH=KVH, G=G, names=args + outs + tuple(scratch))
    smem = pl.BlockSpec(memory_space=pltpu.SMEM)
    anywhere = pl.BlockSpec(memory_space=pltpu.HBM)
    held = pl.BlockSpec(memory_space=pltpu.VMEM)
    grads = pl.pallas_call(
        functools.partial(kernel, sizes),
        out_shape=[
            pltpu.VMEM((KVH, T, G * C), BF16),
            pltpu.VMEM((KVH, T, C), BF16),
            pltpu.VMEM((T, D), BF16),
            pltpu.VMEM((KVH, RO, C), F32),
        ],
        in_specs=[smem, smem] + [anywhere] * 5,
        out_specs=[held] * 4,
        scratch_shapes=list(scratch.values()),
        compiler_params=pltpu.CompilerParams(
            collective_id=0, has_side_effects=True, vmem_limit_bytes=60 * 2**20
        ),
        name="attention_grads",
    )(
        doc_lengths,
        doc_order,
        hidden[0],
        queries[0],
        saved_keys[0],
        grad_out[0],
        value_weight,
    )
    return results(
        grads,
        [
            jax.ShapeDtypeStruct((1, T, QW), BF16),
            jax.ShapeDtypeStruct((1, T, KVW), BF16),
            jax.ShapeDtypeStruct((1, T, D), BF16),
            jax.ShapeDtypeStruct((RO, KVW), F32),
        ],
    )


def results_kernel(query_in, key_in, input_in, weight_in, query, key, x, weight, sems):
    copies = [(input_in, x.at[0])]
    for kv in range(query_in.shape[0]):
        for a, b in ((query_in, query.at[0]), (key_in, key.at[0]), (weight_in, weight)):
            width = a.shape[2]
            copies.append((a.at[kv], b.at[:, pl.ds(kv * width, width)]))
    copies = [pltpu.make_async_copy(a, b, sems.at[i]) for i, (a, b) in enumerate(copies)]
    for copy in copies:
        copy.start()
    for copy in copies:
        copy.wait()


def results(arrays, shapes):
    heads = arrays[0].shape[0]
    return pl.pallas_call(
        results_kernel,
        out_shape=shapes,
        in_specs=[pl.BlockSpec(memory_space=pltpu.VMEM)] * len(arrays),
        out_specs=[pl.BlockSpec(memory_space=pl.ANY)] * len(arrays),
        scratch_shapes=[pltpu.SemaphoreType.DMA((1 + 3 * heads,))],
        compiler_params=pltpu.CompilerParams(vmem_limit_bytes=2**20),
        name="results",
    )(*arrays)


def solution(mesh):
    tokens = P("local", "node", None)
    return jax.shard_map(
        local,
        mesh=mesh,
        in_specs=(tokens,) * 4 + (P("local", None),) * 3,
        out_specs=(tokens,) * 3 + (P(("node", "local"), None),),
        check_vma=False,
    )
```
